32 devices in a mesh: dom: 32 (over z, y, x, core).
Axes of the slice: x: 2, y: 2, z: 4, core: 2. Of those that a mesh axis runs over, the one named last changes fastest.
Arguments:
- displacement: float32 [8, 3, 65536], P(None, None, 'dom'), may hold values from -1.5 to 1.5
- adjoint_disp: float32 [8, 3, 65536], P(None, None, 'dom'), may hold values from -1.5 to 1.5
- pressure: float32 [8, 65536], P(None, 'dom'), may hold values from -3 to 3
- adjoint_pressure: float32 [8, 65536], P(None, 'dom'), may hold values from -3 to 3
- youngs: float32 [65536], P('dom'), may hold values from 0.5 to 2
- permeability: float32 [65536], P('dom'), may hold values from 0.3 to 3
- stiffness: float32 [24, 24], replicated
- send_nodes: int32 [8, 4096], P(None, 'dom'), may hold values from 0 to 2047
- send_cells: int32 [8, 4096], P(None, 'dom'), may hold values from 0 to 2047
- elem_nodes: int32 [8, 65536], P(None, 'dom'), may hold values from 0 to 3071, as said below
- inner_faces: int32 [2, 196608], P(None, 'dom'), may hold values from 0 to 2047
- cross_faces: int32 [2, 32768], P(None, 'dom'), may hold values from 0 to 2047, as said below
Outputs:
- grad_log_youngs: float32 [65536], P('dom')
- grad_log_perm: float32 [65536], P('dom')
The draws below stay inside these ranges and needn't reach their ends.
Inputs may be any that keep to these rules, and one draw needn't show every extreme that they name: `send_nodes`: entries refer to the partition's own nodes; block j of partition c is read by partition c - o_j, with o as in the reference program. `send_cells`: entries refer to the partition's own cells; block j of partition c is read by partition c - o_j. `elem_nodes`: local numbering as in the reference program; a ghost entry j * 128 + g always has d + o_j on the axis. The first 1536 elements of each partition name only its own nodes; corner 0 of each of the last 512 is a ghost node. `cross_faces`: row 0 is an own cell; row 1 is j * 128 + g with d + o_j always on the axis. `inner_faces`: both rows name cells of the same partition.
All inputs are finite; a program needn't handle non-finite values.
Results may differ from the reference program's by a relative error of at most 0.0003.
Values sent between devices are 32-bit elements; how exact they have to be, the bound alone decides.
A program may use at most 192 MiB of HBM per device.

```python
import math
import jax
import jax.numpy as jnp
from jax import lax

EL = 2048
STEPS = 8
NB = 8
DOFS = 24
NL = 2048
EB = 512
GN = 128
GC = 128
FI = 6144
FX = 1024
NODES = 65536
CELLS = 65536
N_DOM = 32


OFFSETS = (1, -1, 2, -2, 4, -4, 8, -8)


def valid_slots(key, device):
    offsets = jnp.array(OFFSETS, dtype=jnp.int32)
    slot_id = jax.random.randint(key, device.shape, 0, NB, dtype=jnp.int32)
    target = device + offsets[slot_id]
    inside = (target >= 0) & (target < N_DOM)
    return jnp.where(inside, slot_id, slot_id ^ 1).astype(jnp.int32)


def draw_elem_nodes(key, part):
    key_list = jax.random.split(jax.random.fold_in(key, 11), 4)
    total_rows = EL * N_DOM
    device = jnp.arange(total_rows, dtype=jnp.int32) // EL
    element = jnp.arange(total_rows, dtype=jnp.int32) % EL
    own_node = jax.random.randint(key_list[0], (8, total_rows), 0, NL, dtype=jnp.int32)
    slot_id = valid_slots(key_list[1], jnp.broadcast_to(device[None, :], (8, total_rows)))
    row_id = jax.random.randint(key_list[2], (8, total_rows), 0, GN, dtype=jnp.int32)
    ghost_node = NL + slot_id * GN + row_id
    chosen = (jax.random.randint(key_list[3], (8, total_rows), 0, 2, dtype=jnp.int32) == 1) | (jnp.arange(8, dtype=jnp.int32)[:, None] == 0)
    edge_rows = element >= EL - EB
    return jnp.where(edge_rows[None, :] & chosen, ghost_node, own_node).astype(jnp.int32)


def draw_cross_faces(key, part):
    key_list = jax.random.split(jax.random.fold_in(key, 23), 3)
    total_rows = FX * N_DOM
    device = jnp.arange(total_rows, dtype=jnp.int32) // FX
    own_cell = jax.random.randint(key_list[0], (total_rows,), 0, EL, dtype=jnp.int32)
    slot_id = valid_slots(key_list[1], device)
    row_id = jax.random.randint(key_list[2], (total_rows,), 0, GC, dtype=jnp.int32)
    return jnp.stack([own_cell, slot_id * GC + row_id]).astype(jnp.int32)


def draw_stiffness(key, part):
    inner_key = jax.random.fold_in(key, 37)
    base = jax.random.normal(inner_key, (DOFS, DOFS), jnp.float32)
    return (jnp.eye(DOFS, dtype=jnp.float32) + 0.5 * (base + base.T) / math.sqrt(2.0 * DOFS)).astype(jnp.float32)


def place_ends(entries, own_key, smallest, top_value):
    place = [jax.random.randint(jax.random.fold_in(own_key, axis), (), 0, length) for axis, length in enumerate(entries.shape)]
    longest = entries.shape.index(max(entries.shape))
    neighbour = place[:longest] + [(place[longest] + 1) % entries.shape[longest]] + place[longest + 1:]
    return entries.at[tuple(place)].set(smallest).at[tuple(neighbour)].set(top_value)


def levels(stream_key, shape, pieces, least, top_value):
    gain, own = 1.0, jax.random.fold_in(stream_key, 6)
    for position, shards_of in pieces:
        draws = jnp.exp(jax.random.uniform(jax.random.fold_in(own, position), (shards_of,), jnp.float32, least / len(pieces), top_value / len(pieces)))
        gain = gain * jnp.repeat(draws, shape[position] // shards_of).reshape([-1 if axis == position else 1 for axis in range(len(shape))])
    return gain


def noise(rng, extent, deviation, bound, cuts=(), kind=jnp.bfloat16):
    values = deviation * jax.random.normal(rng, extent, jnp.float32)
    if cuts:
        values = values * levels(rng, extent, cuts, -0.22, 0.18)
    return jnp.clip(values, -bound, bound).astype(kind)


def setup_inputs(seed: int = 0) -> dict:
    splits = jax.random.split(jax.random.key(seed), 13)
    return {
        "displacement": noise(splits[0], (STEPS, 3, NODES), 0.25, 1.5, ((2, 32),), jnp.float32),
        "adjoint_disp": noise(splits[1], (STEPS, 3, NODES), 0.25, 1.5, ((2, 32),), jnp.float32),
        "pressure": noise(splits[2], (STEPS, CELLS), 0.5, 3.0, ((1, 32),), jnp.float32),
        "adjoint_pressure": noise(splits[3], (STEPS, CELLS), 0.5, 3.0, ((1, 32),), jnp.float32),
        "youngs": jnp.clip(jnp.exp(math.log(2.0) - 1.3862944 * jax.random.uniform(splits[4], (CELLS,), jnp.float32) ** levels(splits[4], (CELLS,), ((0, 32),), -0.2, 0.2)), 0.5, 2.0),
        "permeability": jnp.clip(jnp.exp(math.log(3.0) - 2.3025851 * jax.random.uniform(splits[5], (CELLS,), jnp.float32) ** levels(splits[5], (CELLS,), ((0, 32),), -0.2, 0.2)), 0.3, 3.0),
        "stiffness": draw_stiffness(jax.random.fold_in(splits[12], 71), 0),
        "send_nodes": place_ends(jax.random.randint(splits[7], (NB, GN * N_DOM), 0, NL), jax.random.fold_in(splits[7], 1), 0, NL - 1).astype(jnp.int32),
        "send_cells": place_ends(jax.random.randint(splits[8], (NB, GC * N_DOM), 0, EL), jax.random.fold_in(splits[8], 1), 0, EL - 1).astype(jnp.int32),
        "elem_nodes": draw_elem_nodes(jax.random.fold_in(splits[12], 71), 0),
        "inner_faces": place_ends(jax.random.randint(splits[10], (2, FI * N_DOM), 0, EL), jax.random.fold_in(splits[10], 1), 0, EL - 1).astype(jnp.int32),
        "cross_faces": draw_cross_faces(jax.random.fold_in(splits[12], 71), 0),
    }


OFFSETS = (1, -1, 2, -2, 4, -4, 8, -8)


def face_terms(press_a, press_b, adj_a, adj_b, perm_a, perm_b):
    product = jnp.sum((press_a - press_b) * (adj_a - adj_b), axis=0)
    denominator = (perm_a + perm_b) * (perm_a + perm_b)
    common = 2.0 * perm_a * perm_b * product / denominator
    return common * perm_b, common * perm_a


def reference(displacement, adjoint_disp, pressure, adjoint_pressure, youngs, permeability, stiffness, send_nodes, send_cells, elem_nodes, inner_faces, cross_faces):
    offsets = jnp.array(OFFSETS, dtype=jnp.int32)
    node_blocks = send_nodes.reshape(NB, N_DOM, GN)

    def one_device(device):
        sources = jnp.clip(device + offsets, 0, N_DOM - 1).astype(jnp.int32)
        ghost_nodes = node_blocks[jnp.arange(NB, dtype=jnp.int32), sources] + sources[:, None] * NL
        table = jnp.concatenate([device * NL + jnp.arange(NL, dtype=jnp.int32), ghost_nodes.reshape(-1).astype(jnp.int32)])
        connect = lax.dynamic_slice_in_dim(elem_nodes, (device * EL).astype(jnp.int32), EL, 1)
        global_nodes = table[connect]
        forward = displacement[:, :, global_nodes].reshape(STEPS, DOFS, EL)
        adjoint = adjoint_disp[:, :, global_nodes].reshape(STEPS, DOFS, EL)
        weighted = jnp.einsum("ab,tbe->tae", stiffness, forward, precision=lax.Precision.HIGHEST)
        strain = jnp.sum(adjoint * weighted, axis=(0, 1))
        modulus = lax.dynamic_slice_in_dim(youngs, (device * EL).astype(jnp.int32), EL, 0)
        return -modulus * strain

    grad_youngs = lax.map(one_device, jnp.arange(N_DOM, dtype=jnp.int32)).reshape(-1)

    inner_base = (jnp.arange(FI * N_DOM, dtype=jnp.int32) // FI) * EL
    face_a = inner_faces[0] + inner_base
    face_b = inner_faces[1] + inner_base
    cross_dev = jnp.arange(FX * N_DOM, dtype=jnp.int32) // FX
    slot_id = (cross_faces[1] // GC).astype(jnp.int32)
    row_id = (cross_faces[1] % GC).astype(jnp.int32)
    source = jnp.clip(cross_dev + offsets[slot_id], 0, N_DOM - 1).astype(jnp.int32)
    cross_a = cross_dev * EL + cross_faces[0]
    cross_b = source * EL + send_cells[slot_id, source * GC + row_id]

    term_a, term_b = face_terms(pressure[:, face_a], pressure[:, face_b], adjoint_pressure[:, face_a], adjoint_pressure[:, face_b], permeability[face_a], permeability[face_b])
    shared_a, shared_b = face_terms(pressure[:, cross_a], pressure[:, cross_b], adjoint_pressure[:, cross_a], adjoint_pressure[:, cross_b], permeability[cross_a], permeability[cross_b])
    gradient = jnp.zeros((CELLS,), jnp.float32)
    gradient = gradient.at[face_a].add(term_a).at[face_b].add(term_b)
    gradient = gradient.at[cross_a].add(shared_a).at[cross_b].add(shared_b)
    return grad_youngs, gradient
```

```python
import functools

import jax
import jax.numpy as jnp
from jax import lax
from jax.experimental import pallas as pl
from jax.experimental.pallas import tpu as pltpu
from jax.sharding import PartitionSpec as P

OFFSETS = (1, -1, 2, -2, 4, -4, 8, -8)
MESH = pl.DeviceIdType.MESH
LANES = 128
ROWS = 8
DOFS = 24
WIDE = 256


def pick(table, lo):
    return jnp.take_along_axis(table, lo, axis=1, mode="promise_in_bounds")


def spread(row):
    return jnp.broadcast_to(row, (ROWS, LANES))


def gather(tables, index, first, last):
    lo = index & (LANES - 1)
    hi = index >> 7
    out = None
    for block in range(first, last):
        got = [pick(table(block), lo) for table in tables]
        if out is None:
            out = got
        else:
            here = hi == block
            out = [jnp.where(here, new, old) for new, old in zip(got, out)]
    return out


def onehot(index):
    rows = lax.broadcasted_iota(jnp.int32, (WIDE, LANES), 0).astype(jnp.bfloat16)
    low = (index & (WIDE - 1)).astype(jnp.float32).astype(jnp.bfloat16)
    same = rows == jnp.broadcast_to(low, (WIDE, LANES))
    hot = jnp.where(same, jnp.bfloat16(1), jnp.bfloat16(0))
    return jnp.concatenate([hot, hot], axis=0)


def fill(parts, planes, blocks):
    for block in range(blocks):
        for number in range(0, len(planes), 2):
            both = jnp.concatenate(
                [
                    jnp.concatenate([plane(2 * block), plane(2 * block + 1)], axis=1)
                    for plane in planes[number : number + 2]
                ],
                axis=0,
            )
            top = both.astype(jnp.bfloat16)
            base = (block * len(planes) + number) * ROWS
            parts[base : base + 2 * ROWS, :WIDE] = top
            parts[base : base + 2 * ROWS, WIDE:] = (both - top.astype(jnp.float32)).astype(
                jnp.bfloat16
            )


def multiply(parts, indices, planes, blocks):
    right = jnp.concatenate([onehot(index) for index in indices], axis=1)
    got = jnp.dot(parts[...], right, preferred_element_type=jnp.float32)
    answers = []
    for number, index in enumerate(indices):
        hi = spread(index) >> 8
        mine = got[:, number * LANES : (number + 1) * LANES]
        out = [mine[plane * ROWS : (plane + 1) * ROWS] for plane in range(planes)]
        for block in range(1, blocks):
            here = hi == block
            for plane in range(planes):
                base = (block * planes + plane) * ROWS
                out[plane] = jnp.where(here, mine[base : base + ROWS], out[plane])
        answers.append(out)
    return answers


def scatter(terms, index, height):
    sub_hi = lax.broadcasted_iota(jnp.int32, (height, LANES), 0)
    sub_lo = lax.broadcasted_iota(jnp.int32, (LANES, LANES), 0).astype(jnp.bfloat16)
    left, right = [], []
    for term, where in zip(terms, index):
        top = term.astype(jnp.bfloat16).astype(jnp.float32)
        rest = term - top
        middle = rest.astype(jnp.bfloat16).astype(jnp.float32)
        low = rest - middle
        hi = where >> 7
        lo = (where & (LANES - 1)).astype(jnp.float32)
        for row in range(ROWS):
            cut = slice(row, row + 1)
            mask = jnp.broadcast_to(hi[cut], (height, LANES)) == sub_hi
            parts = [
                jnp.where(mask, jnp.broadcast_to(part[cut], (height, LANES)), 0.0)
                for part in (top, middle, low)
            ]
            left.append(jnp.concatenate(parts, axis=0).astype(jnp.bfloat16))
            same = jnp.broadcast_to(lo[cut].astype(jnp.bfloat16), (LANES, LANES)) == sub_lo
            right.append(jnp.where(same, jnp.bfloat16(1), jnp.bfloat16(0)))
    sums = lax.dot_general(
        jnp.concatenate(left, axis=1),
        jnp.concatenate(right, axis=1),
        (((1,), (1,)), ((), ())),
        preferred_element_type=jnp.float32,
    )
    return sums[:height] + sums[height : 2 * height] + sums[2 * height :]


def face_terms(product, perm_a, perm_b):
    total = perm_a + perm_b
    common = 2.0 * perm_a * perm_b * product / (total * total)
    return common * perm_b, common * perm_a


def kernel(
    count,
    disp,
    adj,
    press,
    adjpress,
    youngs,
    perm,
    stiff,
    send_nodes,
    send_cells,
    elem,
    inner,
    cross,
    out_young,
    out_perm,
    parts,
    cell_parts,
    permtab,
    outbox,
    ghost,
    back,
    returned,
    forward,
    adjoint,
    kron,
    strain,
    face_a,
    face_b,
    send_sem,
    recv_sem,
    back_send,
    back_recv,
):
    me = lax.axis_index("dom")
    slots = len(OFFSETS)
    node_blocks = disp.shape[2] // LANES
    cell_blocks = perm.shape[0]
    elem_blocks = elem.shape[1] // LANES
    edge_blocks = elem_blocks // 4
    inner_rows = inner.shape[1] // LANES
    cross_rows = cross.shape[1] // LANES

    def on_axis(steps):
        return (me + steps >= 0) & (me + steps < count)

    barrier = pltpu.get_barrier_semaphore()
    around = 0
    for slot, offset in enumerate(OFFSETS):
        around += on_axis(offset).astype(jnp.int32)

        @pl.when(on_axis(offset))
        def _():
            pl.semaphore_signal(barrier, inc=1, device_id=(me + offset,), device_id_type=MESH)

        @pl.when(jnp.logical_not(on_axis(-offset)))
        def _():
            returned[slot] = jnp.zeros((1, LANES), jnp.float32)

    for block in range(cell_blocks):
        permtab[block] = spread(perm[block : block + 1, :])
    for row in range(inner_rows):
        cut = slice(row * LANES, (row + 1) * LANES)
        face_a[row : row + 1, :] = inner[0:1, cut]
        face_b[row : row + 1, :] = inner[1:2, cut]
    for row in range(cross_rows):
        cut = slice(row * LANES, (row + 1) * LANES)
        face_a[inner_rows + row : inner_rows + row + 1, :] = cross[0:1, cut]
        face_b[inner_rows + row : inner_rows + row + 1, :] = cross[1:2, cut]

    def plane(number):
        source, comp = (disp, number) if number < 3 else (adj, number - 3)
        return lambda block: source[comp, :, block * LANES : (block + 1) * LANES]

    def cells(source):
        return lambda block: source[:, block * LANES : (block + 1) * LANES]

    planes = [plane(number) for number in range(6)]
    cell_planes = [cells(press), cells(adjpress)]
    perm_plane = [lambda block: permtab[block]]

    side = DOFS * ROWS
    tall = lax.broadcasted_iota(jnp.int32, (side, DOFS), 0) // ROWS
    unknown = lax.broadcasted_iota(jnp.int32, (side, DOFS), 1)
    repeat = jnp.where(tall == unknown, 1.0, 0.0).astype(jnp.bfloat16)
    row_step = lax.broadcasted_iota(jnp.int32, (side, 2 * side), 0) & (ROWS - 1)
    twice = jnp.concatenate([repeat, repeat], axis=0)
    column_step = lax.broadcasted_iota(jnp.int32, (side, 2 * side), 1) & (ROWS - 1)
    whole = stiff[...]
    top = whole.astype(jnp.bfloat16)
    for number, part in enumerate((top, (whole - top.astype(jnp.float32)).astype(jnp.bfloat16))):
        rows = jnp.dot(repeat, part, preferred_element_type=jnp.float32).astype(jnp.bfloat16)
        full = lax.dot_general(
            rows, twice, (((1,), (1,)), ((), ())), preferred_element_type=jnp.float32
        )
        kron[number] = jnp.where(row_step == column_step, full, 0.0).astype(jnp.bfloat16)

    fill(parts, planes, node_blocks // 2)
    fill(cell_parts, cell_planes, cell_blocks // 2)
    for pair in range(0, slots, 2):
        rows = [send_nodes[slot : slot + 1, :] for slot in (pair, pair + 1)]
        nodes = multiply(parts, rows, 6, node_blocks // 2)
        for slot in (pair, pair + 1):
            where = spread(send_cells[slot : slot + 1, :])
            values = gather(cell_planes, where, 0, cell_blocks)
            for number, value in enumerate(nodes[slot - pair] + values):
                outbox[slot, number] = value
    sent_perm = gather(perm_plane, send_cells[...], 0, cell_blocks)[0]
    for slot in range(slots):
        outbox[slot, 8] = spread(sent_perm[slot : slot + 1, :])

    def exchange(source, target, sent, received, side):
        return [
            (
                pltpu.make_async_remote_copy(
                    src_ref=source.at[slot],
                    dst_ref=target.at[slot],
                    send_sem=sent.at[slot],
                    recv_sem=received.at[slot],
                    device_id=(me + side * offset,),
                    device_id_type=MESH,
                ),
                on_axis(side * offset),
                on_axis(-side * offset),
            )
            for slot, offset in enumerate(OFFSETS)
        ]

    def start(copies):
        for copy, to, _ in copies:
            pl.when(to)(copy.start)

    def wait_recv(copies):
        for copy, _, come in copies:
            pl.when(come)(copy.wait_recv)

    def wait_send(copies):
        for copy, to, _ in copies:
            pl.when(to)(copy.wait_send)

    pl.semaphore_wait(barrier, around)
    copies = exchange(outbox, ghost, send_sem, recv_sem, -1)
    start(copies)

    out_perm[...] = jnp.zeros(out_perm.shape, jnp.float32)

    def inner_faces(step, carry):
        base = pl.multiple_of(step * ROWS, ROWS)
        where_a = face_a[pl.ds(base, ROWS), :]
        where_b = face_b[pl.ds(base, ROWS), :]
        products = []
        others = [where_b[row : row + 1] for row in range(ROWS)]
        others = multiply(cell_parts, others, 2, cell_blocks // 2)
        for row in range(ROWS):
            pa, qa = gather(cell_planes, spread(where_a[row : row + 1]), 0, cell_blocks)
            pb, qb = others[row]
            products.append(jnp.sum((pa - pb) * (qa - qb), axis=0, keepdims=True))
        product = jnp.concatenate(products, axis=0)
        perm_a = gather(perm_plane, where_a, 0, cell_blocks)[0]
        perm_b = gather(perm_plane, where_b, 0, cell_blocks)[0]
        term_a, term_b = face_terms(product, perm_a, perm_b)
        out_perm[...] += scatter([term_a, term_b], [where_a, where_b], cell_blocks)
        return carry

    lax.fori_loop(0, inner_rows // ROWS, inner_faces, 0)

    def keep(lanes, values, corner):
        for comp in range(3):
            base = (comp * 8 + corner) * ROWS
            near = slice(base, base + 2 * ROWS)
            both = jnp.concatenate([value[comp] for value in values], axis=0)
            top = both.astype(jnp.bfloat16)
            low = (both - top.astype(jnp.float32)).astype(jnp.bfloat16)
            forward[near, lanes] = top
            forward[DOFS * ROWS + base : DOFS * ROWS + base + 2 * ROWS, lanes] = low
            adjoint[near, lanes] = jnp.concatenate([value[3 + comp] for value in values], axis=0)

    def inner_elements(step, carry):
        lanes = pl.ds(pl.multiple_of(step * LANES, LANES), LANES)
        for corner in range(0, 8, 2):
            rows = [elem[one : one + 1, lanes] for one in (corner, corner + 1)]
            if corner < 6:
                values = multiply(parts, rows, 6, node_blocks // 2)
            else:
                values = [gather(planes, spread(row), 0, node_blocks) for row in rows]
            keep(lanes, values, corner)
        return carry

    lax.fori_loop(0, elem_blocks - edge_blocks, inner_elements, 0)

    wait_recv(copies)

    def ghosts(number):
        return lambda block: ghost[block, number]

    where_a = face_a[inner_rows : inner_rows + cross_rows, :]
    where_b = face_b[inner_rows : inner_rows + cross_rows, :]
    products = []
    own = [where_a[row : row + 1] for row in range(cross_rows)]
    own = multiply(cell_parts, own, 2, cell_blocks // 2)
    for row in range(cross_rows):
        pa, qa = own[row]
        pb, qb = gather([ghosts(6), ghosts(7)], spread(where_b[row : row + 1]), 0, slots)
        products.append(jnp.sum((pa - pb) * (qa - qb), axis=0, keepdims=True))
    product = jnp.concatenate(products, axis=0)
    perm_a = gather(perm_plane, where_a, 0, cell_blocks)[0]
    perm_b = gather([ghosts(8)], where_b, 0, slots)[0]
    term_a, term_b = face_terms(product, perm_a, perm_b)
    owed = scatter([term_b], [where_b], slots)
    for slot in range(slots):
        back[slot] = owed[slot : slot + 1, :]
    out_perm[...] += scatter([term_a], [where_a], cell_blocks)
    backs = exchange(back, returned, back_send, back_recv, 1)
    start(backs)

    far_planes = [ghosts(number) for number in range(6)]

    def edge_elements(step, carry):
        lanes = pl.ds(pl.multiple_of(step * LANES, LANES), LANES)
        for corner in range(0, 8, 2):
            values = []
            rows = [elem[one : one + 1, lanes] for one in (corner, corner + 1)]
            near = multiply(parts, rows, 6, node_blocks // 2)
            for row, mine in zip(rows, near):
                index = spread(row)
                far = gather(far_planes, index - node_blocks * LANES, 0, slots)
                inside = index < node_blocks * LANES
                values.append([jnp.where(inside, a, b) for a, b in zip(mine, far)])
            keep(lanes, values, corner)
        return carry

    lax.fori_loop(elem_blocks - edge_blocks, elem_blocks, edge_elements, 0)

    side = DOFS * ROWS
    wide = elem.shape[1] // 4

    for part in range(4):
        lanes = slice(part * wide, (part + 1) * wide)
        weighted = jnp.dot(kron[0], forward[:, lanes], preferred_element_type=jnp.float32)
        weighted += jnp.dot(
            kron[1, :, :side], forward[:side, lanes], preferred_element_type=jnp.float32
        )
        product = weighted * adjoint[:, lanes]
        sums = jnp.sum(product, axis=0, keepdims=True)
        for row in range(wide // LANES):
            spot = part * (wide // LANES) + row
            strain[spot : spot + 1, :] = sums[:, row * LANES : (row + 1) * LANES]
    out_young[...] = -youngs[...] * strain[...]

    wait_recv(backs)
    arrived = jnp.concatenate([returned[slot] for slot in range(slots)], axis=0)
    out_perm[...] += scatter([arrived], [send_cells[...]], cell_blocks)
    wait_send(copies)
    wait_send(backs)


def on_device(count, *arguments):
    (disp, adj, press, adjpress, youngs, perm, stiff, nodes, cells, elem, inner, cross) = arguments
    blocks = youngs.shape[0] // LANES
    slots = len(OFFSETS)
    face_rows = (inner.shape[1] + cross.shape[1]) // LANES
    vmem = pl.BlockSpec(memory_space=pltpu.VMEM)
    tile = (ROWS, LANES)
    shape = jax.ShapeDtypeStruct((blocks, LANES), jnp.float32)
    young, flow = pl.pallas_call(
        functools.partial(kernel, count),
        out_shape=(shape, shape),
        in_specs=[vmem] * 12,
        out_specs=(vmem, vmem),
        scratch_shapes=[
            pltpu.VMEM((disp.shape[2] // WIDE * 6 * ROWS, 2 * WIDE), jnp.bfloat16),
            pltpu.VMEM((blocks // 2 * 2 * ROWS, 2 * WIDE), jnp.bfloat16),
            pltpu.VMEM((blocks,) + tile, jnp.float32),
            pltpu.VMEM((slots, 9) + tile, jnp.float32),
            pltpu.VMEM((slots, 9) + tile, jnp.float32),
            pltpu.VMEM((slots, 1, LANES), jnp.float32),
            pltpu.VMEM((slots, 1, LANES), jnp.float32),
            pltpu.VMEM((2 * DOFS * ROWS, elem.shape[1]), jnp.bfloat16),
            pltpu.VMEM((DOFS * ROWS, elem.shape[1]), jnp.float32),
            pltpu.VMEM((2, DOFS * ROWS, 2 * DOFS * ROWS), jnp.bfloat16),
            pltpu.VMEM((elem.shape[1] // LANES, LANES), jnp.float32),
            pltpu.VMEM((face_rows, LANES), jnp.int32),
            pltpu.VMEM((face_rows, LANES), jnp.int32),
            pltpu.SemaphoreType.DMA((slots,)),
            pltpu.SemaphoreType.DMA((slots,)),
            pltpu.SemaphoreType.DMA((slots,)),
            pltpu.SemaphoreType.DMA((slots,)),
        ],
        compiler_params=pltpu.CompilerParams(collective_id=0, has_side_effects=True),
    )(
        disp.transpose(1, 0, 2),
        adj.transpose(1, 0, 2),
        press,
        adjpress,
        youngs.reshape(blocks, LANES),
        perm.reshape(blocks, LANES),
        stiff,
        nodes,
        cells,
        elem,
        inner,
        cross,
    )
    return (young.reshape(-1), flow.reshape(-1))


def solution(mesh):
    in_specs = (
        P(None, None, "dom"),
        P(None, None, "dom"),
        P(None, "dom"),
        P(None, "dom"),
        P("dom"),
        P("dom"),
        P(),
        P(None, "dom"),
        P(None, "dom"),
        P(None, "dom"),
        P(None, "dom"),
        P(None, "dom"),
    )
    out_specs = (P("dom"), P("dom"))
    return jax.shard_map(
        functools.partial(on_device, mesh.shape["dom"]),
        mesh=mesh,
        in_specs=in_specs,
        out_specs=out_specs,
        check_vma=False,
    )
```

```python
import functools

import jax
import jax.numpy as jnp
from jax import lax
from jax.experimental import pallas as pl
from jax.experimental.pallas import tpu as pltpu
from jax.sharding import PartitionSpec as P

OFFSETS = (1, -1, 2, -2, 4, -4, 8, -8)
MESH = pl.DeviceIdType.MESH
LANES = 128
ROWS = 8
DOFS = 24
WIDE = 256


def pick(table, lo):
    return jnp.take_along_axis(table, lo, axis=1, mode="promise_in_bounds")


def spread(row):
    return jnp.broadcast_to(row, (ROWS, LANES))


def gather(tables, index, first, last):
    lo = index & (LANES - 1)
    hi = index >> 7
    out = None
    for block in range(first, last):
        got = [pick(table(block), lo) for table in tables]
        if out is None:
            out = got
        else:
            here = hi == block
            out = [jnp.where(here, new, old) for new, old in zip(got, out)]
    return out


def onehot(index):
    rows = lax.broadcasted_iota(jnp.int32, (WIDE, LANES), 0).astype(jnp.bfloat16)
    low = (index & (WIDE - 1)).astype(jnp.float32).astype(jnp.bfloat16)
    same = rows == jnp.broadcast_to(low, (WIDE, LANES))
    hot = jnp.where(same, jnp.bfloat16(1), jnp.bfloat16(0))
    return jnp.concatenate([hot, hot], axis=0)


def fill(parts, planes, blocks):
    for block in range(blocks):
        for number in range(0, len(planes), 2):
            both = jnp.concatenate(
                [
                    jnp.concatenate([plane(2 * block), plane(2 * block + 1)], axis=1)
                    for plane in planes[number : number + 2]
                ],
                axis=0,
            )
            top = both.astype(jnp.bfloat16)
            base = (block * len(planes) + number) * ROWS
            parts[base : base + 2 * ROWS, :WIDE] = top
            parts[base : base + 2 * ROWS, WIDE:] = (both - top.astype(jnp.float32)).astype(
                jnp.bfloat16
            )


def multiply(parts, indices, planes, blocks):
    right = jnp.concatenate([onehot(index) for index in indices], axis=1)
    got = jnp.dot(parts[...], right, preferred_element_type=jnp.float32)
    answers = []
    for number, index in enumerate(indices):
        hi = spread(index) >> 8
        mine = got[:, number * LANES : (number + 1) * LANES]
        out = [mine[plane * ROWS : (plane + 1) * ROWS] for plane in range(planes)]
        for block in range(1, blocks):
            here = hi == block
            for plane in range(planes):
                base = (block * planes + plane) * ROWS
                out[plane] = jnp.where(here, mine[base : base + ROWS], out[plane])
        answers.append(out)
    return answers


def scatter(terms, index, height):
    sub_hi = lax.broadcasted_iota(jnp.int32, (height, LANES), 0)
    sub_lo = lax.broadcasted_iota(jnp.int32, (LANES, LANES), 0).astype(jnp.bfloat16)
    left, right = [], []
    for term, where in zip(terms, index):
        top = term.astype(jnp.bfloat16).astype(jnp.float32)
        rest = term - top
        middle = rest.astype(jnp.bfloat16).astype(jnp.float32)
        low = rest - middle
        hi = where >> 7
        lo = (where & (LANES - 1)).astype(jnp.float32)
        for row in range(ROWS):
            cut = slice(row, row + 1)
            mask = jnp.broadcast_to(hi[cut], (height, LANES)) == sub_hi
            parts = [
                jnp.where(mask, jnp.broadcast_to(part[cut], (height, LANES)), 0.0)
                for part in (top, middle, low)
            ]
            left.append(jnp.concatenate(parts, axis=0).astype(jnp.bfloat16))
            same = jnp.broadcast_to(lo[cut].astype(jnp.bfloat16), (LANES, LANES)) == sub_lo
            right.append(jnp.where(same, jnp.bfloat16(1), jnp.bfloat16(0)))
    sums = lax.dot_general(
        jnp.concatenate(left, axis=1),
        jnp.concatenate(right, axis=1),
        (((1,), (1,)), ((), ())),
        preferred_element_type=jnp.float32,
    )
    return sums[:height] + sums[height : 2 * height] + sums[2 * height :]


def face_terms(product, perm_a, perm_b):
    total = perm_a + perm_b
    common = 2.0 * perm_a * perm_b * product / (total * total)
    return common * perm_b, common * perm_a


def kernel(
    count,
    disp,
    adj,
    press,
    adjpress,
    youngs,
    perm,
    stiff,
    send_nodes,
    send_cells,
    elem,
    inner,
    cross,
    out_young,
    out_perm,
    parts,
    cell_parts,
    permtab,
    outbox,
    ghost,
    back,
    returned,
    forward,
    adjoint,
    kron,
    strain,
    face_a,
    face_b,
    send_sem,
    recv_sem,
    back_send,
    back_recv,
):
    me = lax.axis_index("dom")
    slots = len(OFFSETS)
    node_blocks = disp.shape[2] // LANES
    cell_blocks = perm.shape[0]
    elem_blocks = elem.shape[1] // LANES
    edge_blocks = elem_blocks // 4
    inner_rows = inner.shape[1] // LANES
    cross_rows = cross.shape[1] // LANES

    def on_axis(steps):
        return (me + steps >= 0) & (me + steps < count)

    barrier = pltpu.get_barrier_semaphore()
    around = 0
    for slot, offset in enumerate(OFFSETS):
        around += on_axis(offset).astype(jnp.int32)

        @pl.when(on_axis(offset))
        def _():
            pl.semaphore_signal(barrier, inc=1, device_id=(me + offset,), device_id_type=MESH)

        @pl.when(jnp.logical_not(on_axis(-offset)))
        def _():
            returned[slot] = jnp.zeros((1, LANES), jnp.float32)

    def plane(number):
        source, comp = (disp, number) if number < 3 else (adj, number - 3)
        return lambda block: source[comp, :, block * LANES : (block + 1) * LANES]

    def cells(source):
        return lambda block: source[:, block * LANES : (block + 1) * LANES]

    planes = [plane(number) for number in range(6)]
    cell_planes = [cells(press), cells(adjpress)]
    perm_plane = [lambda block: permtab[block]]

    for block in range(cell_blocks):
        permtab[block] = spread(perm[block : block + 1, :])
    fill(parts, planes, node_blocks // 2)
    fill(cell_parts, cell_planes, cell_blocks // 2)
    for pair in range(0, slots, 2):
        rows = [send_nodes[slot : slot + 1, :] for slot in (pair, pair + 1)]
        nodes = multiply(parts, rows, 6, node_blocks // 2)
        for slot in (pair, pair + 1):
            where = spread(send_cells[slot : slot + 1, :])
            values = gather(cell_planes, where, 0, cell_blocks)
            for number, value in enumerate(nodes[slot - pair] + values):
                outbox[slot, number] = value
    sent_perm = gather(perm_plane, send_cells[...], 0, cell_blocks)[0]
    for slot in range(slots):
        outbox[slot, 8] = spread(sent_perm[slot : slot + 1, :])

    def exchange(source, target, sent, received, side):
        return [
            (
                pltpu.make_async_remote_copy(
                    src_ref=source.at[slot],
                    dst_ref=target.at[slot],
                    send_sem=sent.at[slot],
                    recv_sem=received.at[slot],
                    device_id=(me + side * offset,),
                    device_id_type=MESH,
                ),
                on_axis(side * offset),
                on_axis(-side * offset),
            )
            for slot, offset in enumerate(OFFSETS)
        ]

    def start(copies):
        for copy, to, _ in copies:
            pl.when(to)(copy.start)

    def wait_recv(copies):
        for copy, _, come in copies:
            pl.when(come)(copy.wait_recv)

    def wait_send(copies):
        for copy, to, _ in copies:
            pl.when(to)(copy.wait_send)

    pl.semaphore_wait(barrier, around)
    copies = exchange(outbox, ghost, send_sem, recv_sem, -1)
    start(copies)

    side = DOFS * ROWS
    tall = lax.broadcasted_iota(jnp.int32, (side, DOFS), 0) // ROWS
    unknown = lax.broadcasted_iota(jnp.int32, (side, DOFS), 1)
    repeat = jnp.where(tall == unknown, 1.0, 0.0).astype(jnp.bfloat16)
    row_step = lax.broadcasted_iota(jnp.int32, (side, 2 * side), 0) & (ROWS - 1)
    twice = jnp.concatenate([repeat, repeat], axis=0)
    column_step = lax.broadcasted_iota(jnp.int32, (side, 2 * side), 1) & (ROWS - 1)
    whole = stiff[...]
    top = whole.astype(jnp.bfloat16)
    for number, part in enumerate((top, (whole - top.astype(jnp.float32)).astype(jnp.bfloat16))):
        rows = jnp.dot(repeat, part, preferred_element_type=jnp.float32).astype(jnp.bfloat16)
        full = lax.dot_general(
            rows, twice, (((1,), (1,)), ((), ())), preferred_element_type=jnp.float32
        )
        kron[number] = jnp.where(row_step == column_step, full, 0.0).astype(jnp.bfloat16)

    for row in range(inner_rows):
        cut = slice(row * LANES, (row + 1) * LANES)
        face_a[row : row + 1, :] = inner[0:1, cut]
        face_b[row : row + 1, :] = inner[1:2, cut]
    for row in range(cross_rows):
        cut = slice(row * LANES, (row + 1) * LANES)
        face_a[inner_rows + row : inner_rows + row + 1, :] = cross[0:1, cut]
        face_b[inner_rows + row : inner_rows + row + 1, :] = cross[1:2, cut]

    out_perm[...] = jnp.zeros(out_perm.shape, jnp.float32)

    def inner_faces(step):
        base = pl.multiple_of(step * ROWS, ROWS)
        where_a = face_a[pl.ds(base, ROWS), :]
        where_b = face_b[pl.ds(base, ROWS), :]
        products = []
        others = [where_b[row : row + 1] for row in range(ROWS)]
        others = multiply(cell_parts, others, 2, cell_blocks // 2)
        for row in range(ROWS):
            pa, qa = gather(cell_planes, spread(where_a[row : row + 1]), 0, cell_blocks)
            pb, qb = others[row]
            products.append(jnp.sum((pa - pb) * (qa - qb), axis=0, keepdims=True))
        product = jnp.concatenate(products, axis=0)
        perm_a = gather(perm_plane, where_a, 0, cell_blocks)[0]
        perm_b = gather(perm_plane, where_b, 0, cell_blocks)[0]
        return face_terms(product, perm_a, perm_b), (where_a, where_b)

    def keep(lanes, values, corner):
        for comp in range(3):
            base = (comp * 8 + corner) * ROWS
            near = slice(base, base + 2 * ROWS)
            both = jnp.concatenate([value[comp] for value in values], axis=0)
            top = both.astype(jnp.bfloat16)
            low = (both - top.astype(jnp.float32)).astype(jnp.bfloat16)
            forward[near, lanes] = top
            forward[DOFS * ROWS + base : DOFS * ROWS + base + 2 * ROWS, lanes] = low
            adjoint[near, lanes] = jnp.concatenate([value[3 + comp] for value in values], axis=0)

    def inner_elements(step):
        lanes = pl.ds(pl.multiple_of(step * LANES, LANES), LANES)
        for corner in range(0, 8, 2):
            rows = [elem[one : one + 1, lanes] for one in (corner, corner + 1)]
            if corner < 6:
                values = multiply(parts, rows, 6, node_blocks // 2)
            else:
                values = [gather(planes, spread(row), 0, node_blocks) for row in rows]
            keep(lanes, values, corner)

    face_steps = inner_rows // ROWS
    inner_blocks = elem_blocks - edge_blocks
    each = inner_blocks // face_steps
    assert face_steps * ROWS == inner_rows and each * face_steps == inner_blocks

    def inner(step, carry):
        terms, where = inner_faces(step)
        for number in range(each):
            inner_elements(step * each + number)
            if number == 0:
                out_perm[...] += scatter(terms, where, cell_blocks)
        return carry

    lax.fori_loop(0, face_steps, inner, 0)

    wide = elem.shape[1] // 4

    def strains(part):
        lanes = slice(part * wide, (part + 1) * wide)
        weighted = jnp.dot(kron[0], forward[:, lanes], preferred_element_type=jnp.float32)
        weighted += jnp.dot(
            kron[1, :, :side], forward[:side, lanes], preferred_element_type=jnp.float32
        )
        product = weighted * adjoint[:, lanes]
        sums = jnp.sum(product, axis=0, keepdims=True)
        for row in range(wide // LANES):
            spot = part * (wide // LANES) + row
            strain[spot : spot + 1, :] = sums[:, row * LANES : (row + 1) * LANES]

    wait_recv(copies)

    def ghosts(number):
        return lambda block: ghost[block, number]

    where_a = face_a[inner_rows : inner_rows + cross_rows, :]
    where_b = face_b[inner_rows : inner_rows + cross_rows, :]
    products = []
    own = [where_a[row : row + 1] for row in range(cross_rows)]
    own = multiply(cell_parts, own, 2, cell_blocks // 2)
    for row in range(cross_rows):
        pa, qa = own[row]
        pb, qb = gather([ghosts(6), ghosts(7)], spread(where_b[row : row + 1]), 0, slots)
        products.append(jnp.sum((pa - pb) * (qa - qb), axis=0, keepdims=True))
    product = jnp.concatenate(products, axis=0)
    perm_a = gather(perm_plane, where_a, 0, cell_blocks)[0]
    perm_b = gather([ghosts(8)], where_b, 0, slots)[0]
    term_a, term_b = face_terms(product, perm_a, perm_b)
    strains(0)
    owed = scatter([term_b], [where_b], slots)
    for slot in range(slots):
        back[slot] = owed[slot : slot + 1, :]
    strains(1)
    out_perm[...] += scatter([term_a], [where_a], cell_blocks)
    strains(2)
    backs = exchange(back, returned, back_send, back_recv, 1)
    start(backs)

    far_planes = [ghosts(number) for number in range(6)]

    def edge_elements(step):
        lanes = pl.ds(pl.multiple_of(step * LANES, LANES), LANES)
        for corner in range(0, 8, 2):
            values = []
            rows = [elem[one : one + 1, lanes] for one in (corner, corner + 1)]
            near = multiply(parts, rows, 6, node_blocks // 2)
            for row, mine in zip(rows, near):
                index = spread(row)
                far = gather(far_planes, index - node_blocks * LANES, 0, slots)
                inside = index < node_blocks * LANES
                values.append([jnp.where(inside, a, b) for a, b in zip(mine, far)])
            keep(lanes, values, corner)

    def edge(step, carry):
        for number in range(2):
            edge_elements(inner_blocks + 2 * step + number)
        return carry

    lax.fori_loop(0, edge_blocks // 2, edge, 0)

    wait_recv(backs)
    arrived = jnp.concatenate([returned[slot] for slot in range(slots)], axis=0)
    strains(3)
    out_perm[...] += scatter([arrived], [send_cells[...]], cell_blocks)
    out_young[...] = -youngs[...] * strain[...]
    wait_send(copies)
    wait_send(backs)


def on_device(count, *arguments):
    (disp, adj, press, adjpress, youngs, perm, stiff, nodes, cells, elem, inner, cross) = arguments
    blocks = youngs.shape[0] // LANES
    slots = len(OFFSETS)
    face_rows = (inner.shape[1] + cross.shape[1]) // LANES
    vmem = pl.BlockSpec(memory_space=pltpu.VMEM)
    tile = (ROWS, LANES)
    shape = jax.ShapeDtypeStruct((blocks, LANES), jnp.float32)
    young, flow = pl.pallas_call(
        functools.partial(kernel, count),
        out_shape=(shape, shape),
        in_specs=[vmem] * 12,
        out_specs=(vmem, vmem),
        scratch_shapes=[
            pltpu.VMEM((disp.shape[2] // WIDE * 6 * ROWS, 2 * WIDE), jnp.bfloat16),
            pltpu.VMEM((blocks // 2 * 2 * ROWS, 2 * WIDE), jnp.bfloat16),
            pltpu.VMEM((blocks,) + tile, jnp.float32),
            pltpu.VMEM((slots, 9) + tile, jnp.float32),
            pltpu.VMEM((slots, 9) + tile, jnp.float32),
            pltpu.VMEM((slots, 1, LANES), jnp.float32),
            pltpu.VMEM((slots, 1, LANES), jnp.float32),
            pltpu.VMEM((2 * DOFS * ROWS, elem.shape[1]), jnp.bfloat16),
            pltpu.VMEM((DOFS * ROWS, elem.shape[1]), jnp.float32),
            pltpu.VMEM((2, DOFS * ROWS, 2 * DOFS * ROWS), jnp.bfloat16),
            pltpu.VMEM((elem.shape[1] // LANES, LANES), jnp.float32),
            pltpu.VMEM((face_rows, LANES), jnp.int32),
            pltpu.VMEM((face_rows, LANES), jnp.int32),
            pltpu.SemaphoreType.DMA((slots,)),
            pltpu.SemaphoreType.DMA((slots,)),
            pltpu.SemaphoreType.DMA((slots,)),
            pltpu.SemaphoreType.DMA((slots,)),
        ],
        compiler_params=pltpu.CompilerParams(collective_id=0, has_side_effects=True),
    )(
        disp.transpose(1, 0, 2),
        adj.transpose(1, 0, 2),
        press,
        adjpress,
        youngs.reshape(blocks, LANES),
        perm.reshape(blocks, LANES),
        stiff,
        nodes,
        cells,
        elem,
        inner,
        cross,
    )
    return (young.reshape(-1), flow.reshape(-1))


def solution(mesh):
    in_specs = (
        P(None, None, "dom"),
        P(None, None, "dom"),
        P(None, "dom"),
        P(None, "dom"),
        P("dom"),
        P("dom"),
        P(),
        P(None, "dom"),
        P(None, "dom"),
        P(None, "dom"),
        P(None, "dom"),
        P(None, "dom"),
    )
    out_specs = (P("dom"), P("dom"))
    return jax.shard_map(
        functools.partial(on_device, mesh.shape["dom"]),
        mesh=mesh,
        in_specs=in_specs,
        out_specs=out_specs,
        check_vma=False,
    )
```

```python
import functools

import jax
import jax.numpy as jnp
from jax import lax
from jax.experimental import pallas as pl
from jax.experimental.pallas import tpu as pltpu
from jax.sharding import PartitionSpec as P

OFFSETS = (1, -1, 2, -2, 4, -4, 8, -8)
MESH = pl.DeviceIdType.MESH
LANES = 128
ROWS = 8
DOFS = 24
WIDE = 256


def pick(table, lo):
    return jnp.take_along_axis(table, lo, axis=1, mode="promise_in_bounds")


def spread(row):
    return jnp.broadcast_to(row, (ROWS, LANES))


def gather(tables, index, first, last):
    lo = index & (LANES - 1)
    hi = index >> 7
    out = None
    for block in range(first, last):
        got = [pick(table(block), lo) for table in tables]
        if out is None:
            out = got
        else:
            here = hi == block
            out = [jnp.where(here, new, old) for new, old in zip(got, out)]
    return out


def onehot(index):
    rows = lax.broadcasted_iota(jnp.int32, (WIDE, LANES), 0).astype(jnp.bfloat16)
    low = (index & (WIDE - 1)).astype(jnp.float32).astype(jnp.bfloat16)
    same = rows == jnp.broadcast_to(low, (WIDE, LANES))
    hot = jnp.where(same, jnp.bfloat16(1), jnp.bfloat16(0))
    return jnp.concatenate([hot, hot], axis=0)


def fill(parts, planes, blocks):
    for block in range(blocks):
        for number in range(0, len(planes), 2):
            both = jnp.concatenate(
                [
                    jnp.concatenate([plane(2 * block), plane(2 * block + 1)], axis=1)
                    for plane in planes[number : number + 2]
                ],
                axis=0,
            )
            top = both.astype(jnp.bfloat16)
            base = (block * len(planes) + number) * ROWS
            parts[base : base + 2 * ROWS, :WIDE] = top
            parts[base : base + 2 * ROWS, WIDE:] = (both - top.astype(jnp.float32)).astype(
                jnp.bfloat16
            )


def multiply(parts, indices, planes, blocks):
    right = jnp.concatenate([onehot(index) for index in indices], axis=1)
    got = jnp.dot(parts[...], right, preferred_element_type=jnp.float32)
    answers = []
    for number, index in enumerate(indices):
        hi = spread(index) >> 8
        mine = got[:, number * LANES : (number + 1) * LANES]
        out = [mine[plane * ROWS : (plane + 1) * ROWS] for plane in range(planes)]
        for block in range(1, blocks):
            here = hi == block
            for plane in range(planes):
                base = (block * planes + plane) * ROWS
                out[plane] = jnp.where(here, mine[base : base + ROWS], out[plane])
        answers.append(out)
    return answers


def scatter(terms, index, height):
    sub_hi = lax.broadcasted_iota(jnp.int32, (height, LANES), 0)
    sub_lo = lax.broadcasted_iota(jnp.int32, (LANES, LANES), 0).astype(jnp.bfloat16)
    left, right = [], []
    for term, where in zip(terms, index):
        top = term.astype(jnp.bfloat16).astype(jnp.float32)
        rest = term - top
        middle = rest.astype(jnp.bfloat16).astype(jnp.float32)
        low = rest - middle
        hi = where >> 7
        lo = (where & (LANES - 1)).astype(jnp.float32)
        for row in range(ROWS):
            cut = slice(row, row + 1)
            mask = jnp.broadcast_to(hi[cut], (height, LANES)) == sub_hi
            parts = [
                jnp.where(mask, jnp.broadcast_to(part[cut], (height, LANES)), 0.0)
                for part in (top, middle, low)
            ]
            left.append(jnp.concatenate(parts, axis=0).astype(jnp.bfloat16))
            same = jnp.broadcast_to(lo[cut].astype(jnp.bfloat16), (LANES, LANES)) == sub_lo
            right.append(jnp.where(same, jnp.bfloat16(1), jnp.bfloat16(0)))
    sums = lax.dot_general(
        jnp.concatenate(left, axis=1),
        jnp.concatenate(right, axis=1),
        (((1,), (1,)), ((), ())),
        preferred_element_type=jnp.float32,
    )
    return sums[:height] + sums[height : 2 * height] + sums[2 * height :]


def face_terms(product, perm_a, perm_b):
    total = perm_a + perm_b
    common = 2.0 * perm_a * perm_b * product / (total * total)
    return common * perm_b, common * perm_a


def kernel(count, first, second, *refs):
    arguments, refs = refs[:12], refs[12:]
    out, refs = refs[0], refs[1:]
    out_young, out_perm = out.at[0], out.at[1]
    (disp, adj, press, adjpress, youngs, perm), refs = refs[:6], refs[6:]
    (stiff, send_nodes, send_cells, elem, inner, cross), refs = refs[:6], refs[6:]
    (
    parts,
    cell_parts,
    permtab,
    outbox,
    ghost,
    back,
    returned,
    forward,
    adjoint,
    kron,
    strain,
    face_a,
    face_b,
    send_sem,
    recv_sem,
 back_send,
    back_recv,
    load_sem,
    ) = refs
    held = (disp, adj, press, adjpress, youngs, perm)
    held += (stiff, send_nodes, send_cells, elem, inner, cross)
    loads = [
        pltpu.make_async_copy(source, target, load_sem.at[number])
        for number, (source, target) in enumerate(zip(arguments, held))
    ]
    for load in loads:
        load.start()
    me = lax.axis_index("dom")
    slots = len(OFFSETS)
    node_blocks = disp.shape[2] // LANES
    cell_blocks = perm.shape[0]
    elem_blocks = elem.shape[1] // LANES
    edge_blocks = elem_blocks // 4
    inner_rows = inner.shape[1] // LANES
    cross_rows = cross.shape[1] // LANES

    def on_axis(steps):
        return (me + steps >= 0) & (me + steps < count)

    barrier = pltpu.get_barrier_semaphore()
    around = 0
    for slot, offset in enumerate(OFFSETS):
        around += on_axis(offset).astype(jnp.int32)

        @pl.when(on_axis(offset))
        def _():
            pl.semaphore_signal(barrier, inc=1, device_id=(me + offset,), device_id_type=MESH)

        @pl.when(jnp.logical_not(on_axis(-offset)))
        def _():
            returned[slot] = jnp.zeros((1, LANES), jnp.float32)

    def plane(number):
        source, comp = (disp, number) if number < 3 else (adj, number - 3)
        return lambda block: source[comp, :, block * LANES : (block + 1) * LANES]

    def cells(source):
        return lambda block: source[:, block * LANES : (block + 1) * LANES]

    planes = [plane(number) for number in range(6)]
    cell_planes = [cells(press), cells(adjpress)]
    perm_plane = [lambda block: permtab[block]]

    for number in (2, 3, 7, 8, 5, 0, 1, 6, 9, 10, 11, 4):
        loads[number].wait()

    for block in range(cell_blocks):
        permtab[block] = spread(perm[block : block + 1, :])
    fill(parts, planes, node_blocks // 2)
    fill(cell_parts, cell_planes, cell_blocks // 2)
    for pair in range(0, slots, 2):
        rows = [send_nodes[slot : slot + 1, :] for slot in (pair, pair + 1)]
        nodes = multiply(parts, rows, 6, node_blocks // 2)
        for slot in (pair, pair + 1):
            where = spread(send_cells[slot : slot + 1, :])
            values = gather(cell_planes, where, 0, cell_blocks)
            for number, value in enumerate(nodes[slot - pair] + values):
                outbox[slot, number] = value
    sent_perm = gather(perm_plane, send_cells[...], 0, cell_blocks)[0]
    for slot in range(slots):
        outbox[slot, 8] = spread(sent_perm[slot : slot + 1, :])

    def exchange(source, target, sent, received, side):
        return [
            (
                pltpu.make_async_remote_copy(
                    src_ref=source.at[slot],
                    dst_ref=target.at[slot],
                    send_sem=sent.at[slot],
                    recv_sem=received.at[slot],
                    device_id=(me + side * offset,),
                    device_id_type=MESH,
                ),
                on_axis(side * offset),
                on_axis(-side * offset),
            )
            for slot, offset in enumerate(OFFSETS)
        ]

    def start(copies):
        for copy, to, _ in copies:
            pl.when(to)(copy.start)

    def wait_recv(copies):
        for copy, _, come in copies:
            pl.when(come)(copy.wait_recv)

    def wait_send(copies):
        for copy, to, _ in copies:
            pl.when(to)(copy.wait_send)

    side = DOFS * ROWS
    tall = lax.broadcasted_iota(jnp.int32, (side, DOFS), 0) // ROWS
    unknown = lax.broadcasted_iota(jnp.int32, (side, DOFS), 1)
    repeat = jnp.where(tall == unknown, 1.0, 0.0).astype(jnp.bfloat16)
    row_step = lax.broadcasted_iota(jnp.int32, (side, 2 * side), 0) & (ROWS - 1)
    twice = jnp.concatenate([repeat, repeat], axis=0)
    column_step = lax.broadcasted_iota(jnp.int32, (side, 2 * side), 1) & (ROWS - 1)
    whole = stiff[...]
    top = whole.astype(jnp.bfloat16)
    for number, part in enumerate((top, (whole - top.astype(jnp.float32)).astype(jnp.bfloat16))):
        rows = jnp.dot(repeat, part, preferred_element_type=jnp.float32).astype(jnp.bfloat16)
        full = lax.dot_general(
            rows, twice, (((1,), (1,)), ((), ())), preferred_element_type=jnp.float32
        )
        kron[number] = jnp.where(row_step == column_step, full, 0.0).astype(jnp.bfloat16)

    for row in range(inner_rows):
        cut = slice(row * LANES, (row + 1) * LANES)
        face_a[row : row + 1, :] = inner[0:1, cut]
        face_b[row : row + 1, :] = inner[1:2, cut]
    for row in range(cross_rows):
        cut = slice(row * LANES, (row + 1) * LANES)
        face_a[inner_rows + row : inner_rows + row + 1, :] = cross[0:1, cut]
        face_b[inner_rows + row : inner_rows + row + 1, :] = cross[1:2, cut]

    out_perm[...] = jnp.zeros(out_perm.shape, jnp.float32)

    def inner_faces(step):
        base = pl.multiple_of(step * ROWS, ROWS)
        where_a = face_a[pl.ds(base, ROWS), :]
        where_b = face_b[pl.ds(base, ROWS), :]
        products = []
        others = [where_b[row : row + 1] for row in range(ROWS)]
        others = multiply(cell_parts, others, 2, cell_blocks // 2)
        for row in range(ROWS):
            pa, qa = gather(cell_planes, spread(where_a[row : row + 1]), 0, cell_blocks)
            pb, qb = others[row]
            products.append(jnp.sum((pa - pb) * (qa - qb), axis=0, keepdims=True))
        product = jnp.concatenate(products, axis=0)
        perm_a = gather(perm_plane, where_a, 0, cell_blocks)[0]
        perm_b = gather(perm_plane, where_b, 0, cell_blocks)[0]
        return face_terms(product, perm_a, perm_b), (where_a, where_b)

    def keep(lanes, values, corner):
        for comp in range(3):
            base = (comp * 8 + corner) * ROWS
            near = slice(base, base + 2 * ROWS)
            both = jnp.concatenate([value[comp] for value in values], axis=0)
            top = both.astype(jnp.bfloat16)
            low = (both - top.astype(jnp.float32)).astype(jnp.bfloat16)
            forward[near, lanes] = top
            forward[DOFS * ROWS + base : DOFS * ROWS + base + 2 * ROWS, lanes] = low
            adjoint[near, lanes] = jnp.concatenate([value[3 + comp] for value in values], axis=0)

    def inner_elements(step):
        lanes = pl.ds(pl.multiple_of(step * LANES, LANES), LANES)
        for corner in range(0, 8, 2):
            rows = [elem[one : one + 1, lanes] for one in (corner, corner + 1)]
            if corner < 6:
                values = multiply(parts, rows, 6, node_blocks // 2)
            else:
                values = [gather(planes, spread(row), 0, node_blocks) for row in rows]
            keep(lanes, values, corner)

    face_steps = inner_rows // ROWS
    inner_blocks = elem_blocks - edge_blocks
    each = inner_blocks // face_steps
    assert face_steps * ROWS == inner_rows and each * face_steps == inner_blocks

    def inner(step, carry):
        terms, where = inner_faces(step)
        for number in range(each):
            inner_elements(step * each + number)
            if number == 0:
                out_perm[...] += scatter(terms, where, cell_blocks)
        return carry

    lax.fori_loop(0, first, inner, 0)

    pl.semaphore_wait(barrier, around)
    copies = exchange(outbox, ghost, send_sem, recv_sem, -1)
    start(copies)

    lax.fori_loop(first, second, inner, 0)

    wide = elem.shape[1] // 4

    def strains(part):
        lanes = slice(part * wide, (part + 1) * wide)
        weighted = jnp.dot(kron[0], forward[:, lanes], preferred_element_type=jnp.float32)
        weighted += jnp.dot(
            kron[1, :, :side], forward[:side, lanes], preferred_element_type=jnp.float32
        )
        product = weighted * adjoint[:, lanes]
        sums = jnp.sum(product, axis=0, keepdims=True)
        for row in range(wide // LANES):
            spot = part * (wide // LANES) + row
            strain[spot : spot + 1, :] = sums[:, row * LANES : (row + 1) * LANES]

    wait_recv(copies)

    def ghosts(number):
        return lambda block: ghost[block, number]

    where_a = face_a[inner_rows : inner_rows + cross_rows, :]
    where_b = face_b[inner_rows : inner_rows + cross_rows, :]
    products = []
    own = [where_a[row : row + 1] for row in range(cross_rows)]
    own = multiply(cell_parts, own, 2, cell_blocks // 2)
    for row in range(cross_rows):
        pa, qa = own[row]
        pb, qb = gather([ghosts(6), ghosts(7)], spread(where_b[row : row + 1]), 0, slots)
        products.append(jnp.sum((pa - pb) * (qa - qb), axis=0, keepdims=True))
    product = jnp.concatenate(products, axis=0)
    perm_a = gather(perm_plane, where_a, 0, cell_blocks)[0]
    perm_b = gather([ghosts(8)], where_b, 0, slots)[0]
    term_a, term_b = face_terms(product, perm_a, perm_b)
    strains(0)
    owed = scatter([term_b], [where_b], slots)
    for slot in range(slots):
        back[slot] = owed[slot : slot + 1, :]
    strains(1)
    out_perm[...] += scatter([term_a], [where_a], cell_blocks)
    backs = exchange(back, returned, back_send, back_recv, 1)
    start(backs)

    lax.fori_loop(second, face_steps, inner, 0)

    far_planes = [ghosts(number) for number in range(6)]

    def edge_elements(step):
        lanes = pl.ds(pl.multiple_of(step * LANES, LANES), LANES)
        for corner in range(0, 8, 2):
            values = []
            rows = [elem[one : one + 1, lanes] for one in (corner, corner + 1)]
            near = multiply(parts, rows, 6, node_blocks // 2)
            for row, mine in zip(rows, near):
                index = spread(row)
                far = gather(far_planes, index - node_blocks * LANES, 0, slots)
                inside = index < node_blocks * LANES
                values.append([jnp.where(inside, a, b) for a, b in zip(mine, far)])
            keep(lanes, values, corner)

    def edge(step, carry):
        for number in range(2):
            edge_elements(inner_blocks + 2 * step + number)
        return carry

    lax.fori_loop(0, edge_blocks // 2, edge, 0)

    wait_recv(backs)
    arrived = jnp.concatenate([returned[slot] for slot in range(slots)], axis=0)
    strains(2)
    strains(3)
    out_perm[...] += scatter([arrived], [send_cells[...]], cell_blocks)
    out_young[...] = -youngs[...] * strain[...]
    wait_send(copies)
    wait_send(backs)


def deliver(both, young, flow, sem):
    copies = [
        pltpu.make_async_copy(both.at[number], target, sem.at[number])
        for number, target in enumerate((young, flow))
    ]
    for copy in copies:
        copy.start()
    for copy in copies:
        copy.wait()


def on_device(count, *arguments):
    (disp, adj, press, adjpress, youngs, perm, stiff, nodes, cells, elem, inner, cross) = arguments
    blocks = youngs.shape[0] // LANES
    slots = len(OFFSETS)
    face_rows = (inner.shape[1] + cross.shape[1]) // LANES
    vmem = pl.BlockSpec(memory_space=pltpu.VMEM)
    tile = (ROWS, LANES)
    shape = jax.ShapeDtypeStruct((blocks, LANES), jnp.float32)
    operands = (
        disp.transpose(1, 0, 2),
        adj.transpose(1, 0, 2),
        press,
        adjpress,
        youngs.reshape(blocks, LANES),
        perm.reshape(blocks, LANES),
        stiff,
        nodes,
        cells,
        elem,
        inner,
        cross,
    )
    both = pl.pallas_call(
        functools.partial(kernel, count, 1, 5),
        out_shape=pltpu.VMEM((2, blocks, LANES), jnp.float32),
        in_specs=[pl.BlockSpec(memory_space=pltpu.HBM)] * 12,
        out_specs=vmem,
        scratch_shapes=[pltpu.VMEM(one.shape, one.dtype) for one in operands]
        + [
            pltpu.VMEM((disp.shape[2] // WIDE * 6 * ROWS, 2 * WIDE), jnp.bfloat16),
            pltpu.VMEM((blocks // 2 * 2 * ROWS, 2 * WIDE), jnp.bfloat16),
            pltpu.VMEM((blocks,) + tile, jnp.float32),
            pltpu.VMEM((slots, 9) + tile, jnp.float32),
            pltpu.VMEM((slots, 9) + tile, jnp.float32),
            pltpu.VMEM((slots, 1, LANES), jnp.float32),
            pltpu.VMEM((slots, 1, LANES), jnp.float32),
            pltpu.VMEM((2 * DOFS * ROWS, elem.shape[1]), jnp.bfloat16),
            pltpu.VMEM((DOFS * ROWS, elem.shape[1]), jnp.float32),
            pltpu.VMEM((2, DOFS * ROWS, 2 * DOFS * ROWS), jnp.bfloat16),
            pltpu.VMEM((elem.shape[1] // LANES, LANES), jnp.float32),
            pltpu.VMEM((face_rows, LANES), jnp.int32),
            pltpu.VMEM((face_rows, LANES), jnp.int32),
            pltpu.SemaphoreType.DMA((slots,)),
            pltpu.SemaphoreType.DMA((slots,)),
            pltpu.SemaphoreType.DMA((slots,)),
            pltpu.SemaphoreType.DMA((slots,)),
            pltpu.SemaphoreType.DMA((len(operands),)),
        ],
        compiler_params=pltpu.CompilerParams(
            collective_id=0, has_side_effects=True),
    )(*operands)
    size = blocks * LANES
    whole = jax.ShapeDtypeStruct((blocks, LANES), jnp.float32)
    anywhere = pl.BlockSpec(memory_space=pl.ANY)
    young, flow = pl.pallas_call(
        deliver,
        out_shape=(whole, whole),
        in_specs=[vmem],
        out_specs=(anywhere, anywhere),
        scratch_shapes=[pltpu.SemaphoreType.DMA((2,))],
        compiler_params=pltpu.CompilerParams(vmem_limit_bytes=2**20),
    )(both)
    return (young.reshape(-1), flow.reshape(-1))


def solution(mesh):
    in_specs = (
        P(None, None, "dom"),
        P(None, None, "dom"),
        P(None, "dom"),
        P(None, "dom"),
        P("dom"),
        P("dom"),
        P(),
        P(None, "dom"),
        P(None, "dom"),
        P(None, "dom"),
        P(None, "dom"),
        P(None, "dom"),
    )
    out_specs = (P("dom"), P("dom"))
    return jax.shard_map(
        functools.partial(on_device, mesh.shape["dom"]),
        mesh=mesh,
        in_specs=in_specs,
        out_specs=out_specs,
        check_vma=False,
    )
```

```python
import functools

import jax
import jax.numpy as jnp
from jax import lax
from jax.experimental import pallas as pl
from jax.experimental.pallas import tpu as pltpu
from jax.sharding import PartitionSpec as P

OFFSETS = (1, -1, 2, -2, 4, -4, 8, -8)
MESH = pl.DeviceIdType.MESH
LANES = 128
ROWS = 8
DOFS = 24
WIDE = 256


def pick(table, lo):
    return jnp.take_along_axis(table, lo, axis=1, mode="promise_in_bounds")


def spread(row):
    return jnp.broadcast_to(row, (ROWS, LANES))


def gather(tables, index, first, last):
    lo = index & (LANES - 1)
    hi = index >> 7
    out = None
    for block in range(first, last):
        got = [pick(table(block), lo) for table in tables]
        if out is None:
            out = got
        else:
            here = hi == block
            out = [jnp.where(here, new, old) for new, old in zip(got, out)]
    return out


def onehot(index):
    rows = lax.broadcasted_iota(jnp.int32, (WIDE, LANES), 0).astype(jnp.bfloat16)
    low = (index & (WIDE - 1)).astype(jnp.float32).astype(jnp.bfloat16)
    same = rows == jnp.broadcast_to(low, (WIDE, LANES))
    hot = jnp.where(same, jnp.bfloat16(1), jnp.bfloat16(0))
    return jnp.concatenate([hot, hot], axis=0)


def fill(parts, planes, blocks):
    for block in range(blocks):
        for number in range(0, len(planes), 2):
            both = jnp.concatenate(
                [
                    jnp.concatenate([plane(2 * block), plane(2 * block + 1)], axis=1)
                    for plane in planes[number : number + 2]
                ],
                axis=0,
            )
            top = both.astype(jnp.bfloat16)
            base = (block * len(planes) + number) * ROWS
            parts[base : base + 2 * ROWS, :WIDE] = top
            parts[base : base + 2 * ROWS, WIDE:] = (both - top.astype(jnp.float32)).astype(
                jnp.bfloat16
            )


def multiply(parts, indices, planes, blocks):
    right = jnp.concatenate([onehot(index) for index in indices], axis=1)
    got = jnp.dot(parts[...], right, preferred_element_type=jnp.float32)
    answers = []
    for number, index in enumerate(indices):
        hi = spread(index) >> 8
        mine = got[:, number * LANES : (number + 1) * LANES]
        out = [mine[plane * ROWS : (plane + 1) * ROWS] for plane in range(planes)]
        for block in range(1, blocks):
            here = hi == block
            for plane in range(planes):
                base = (block * planes + plane) * ROWS
                out[plane] = jnp.where(here, mine[base : base + ROWS], out[plane])
        answers.append(out)
    return answers


def scatter(terms, index, height):
    sub_hi = lax.broadcasted_iota(jnp.int32, (height, LANES), 0)
    sub_lo = lax.broadcasted_iota(jnp.int32, (LANES, LANES), 0).astype(jnp.bfloat16)
    left, right = [], []
    for term, where in zip(terms, index):
        top = term.astype(jnp.bfloat16).astype(jnp.float32)
        rest = term - top
        middle = rest.astype(jnp.bfloat16).astype(jnp.float32)
        low = rest - middle
        hi = where >> 7
        lo = (where & (LANES - 1)).astype(jnp.float32)
        for row in range(ROWS):
            cut = slice(row, row + 1)
            mask = jnp.broadcast_to(hi[cut], (height, LANES)) == sub_hi
            parts = [
                jnp.where(mask, jnp.broadcast_to(part[cut], (height, LANES)), 0.0)
                for part in (top, middle, low)
            ]
            left.append(jnp.concatenate(parts, axis=0).astype(jnp.bfloat16))
            same = jnp.broadcast_to(lo[cut].astype(jnp.bfloat16), (LANES, LANES)) == sub_lo
            right.append(jnp.where(same, jnp.bfloat16(1), jnp.bfloat16(0)))
    sums = lax.dot_general(
        jnp.concatenate(left, axis=1),
        jnp.concatenate(right, axis=1),
        (((1,), (1,)), ((), ())),
        preferred_element_type=jnp.float32,
    )
    return sums[:height] + sums[height : 2 * height] + sums[2 * height :]


def face_terms(product, perm_a, perm_b):
    total = perm_a + perm_b
    common = 2.0 * perm_a * perm_b * product / (total * total)
    return common * perm_b, common * perm_a


def kernel(count, *refs):
    arguments, refs = refs[:12], refs[12:]
    out, refs = refs[0], refs[1:]
    out_young, out_perm = out.at[0], out.at[1]
    (disp, adj, press, adjpress, youngs, perm), refs = refs[:6], refs[6:]
    (stiff, send_nodes, send_cells, elem, inner, cross), refs = refs[:6], refs[6:]
    (
    parts,
    cell_parts,
    permtab,
    node_box,
    cell_box,
    ghost_nodes,
    ghost_cells,
    back,
    returned,
    forward,
    adjoint,
    kron,
    strain,
    face_a,
    face_b,
    node_send,
    node_recv,
    cell_send,
    cell_recv,
 back_send,
    back_recv,
    load_sem,
    ) = refs
    held = (disp, adj, press, adjpress, youngs, perm)
    held += (stiff, send_nodes, send_cells, elem, inner, cross)
    loads = [
        pltpu.make_async_copy(source, target, load_sem.at[number])
        for number, (source, target) in enumerate(zip(arguments, held))
    ]
    for load in loads:
        load.start()
    me = lax.axis_index("dom")
    slots = len(OFFSETS)
    node_blocks = disp.shape[2] // LANES
    cell_blocks = perm.shape[0]
    elem_blocks = elem.shape[1] // LANES
    edge_blocks = elem_blocks // 4
    inner_rows = inner.shape[1] // LANES
    cross_rows = cross.shape[1] // LANES

    def on_axis(steps):
        return (me + steps >= 0) & (me + steps < count)

    barrier = pltpu.get_barrier_semaphore()
    around = 0
    for slot, offset in enumerate(OFFSETS):
        around += on_axis(offset).astype(jnp.int32)

        @pl.when(on_axis(offset))
        def _():
            pl.semaphore_signal(barrier, inc=1, device_id=(me + offset,), device_id_type=MESH)

        @pl.when(jnp.logical_not(on_axis(-offset)))
        def _():
            returned[slot] = jnp.zeros((1, LANES), jnp.float32)

    def plane(number):
        source, comp = (disp, number) if number < 3 else (adj, number - 3)
        return lambda block: source[comp, :, block * LANES : (block + 1) * LANES]

    def cells(source):
        return lambda block: source[:, block * LANES : (block + 1) * LANES]

    planes = [plane(number) for number in range(6)]
    cell_planes = [cells(press), cells(adjpress)]
    perm_plane = [lambda block: permtab[block]]

    for number in (2, 3, 7, 8, 5, 0, 1, 6, 9, 10, 11, 4):
        loads[number].wait()

    for block in range(cell_blocks):
        permtab[block] = spread(perm[block : block + 1, :])
    fill(parts, planes, node_blocks // 2)
    fill(cell_parts, cell_planes, cell_blocks // 2)
    for pair in range(0, slots, 2):
        rows = [send_nodes[slot : slot + 1, :] for slot in (pair, pair + 1)]
        nodes = multiply(parts, rows, 6, node_blocks // 2)
        for slot in (pair, pair + 1):
            where = spread(send_cells[slot : slot + 1, :])
            values = gather(cell_planes, where, 0, cell_blocks)
            for number, value in enumerate(nodes[slot - pair]):
                node_box[slot, number] = value
            for number, value in enumerate(values):
                cell_box[slot, number] = value
    sent_perm = gather(perm_plane, send_cells[...], 0, cell_blocks)[0]
    for slot in range(slots):
        cell_box[slot, 2] = spread(sent_perm[slot : slot + 1, :])

    def exchange(source, target, sent, received, side):
        return [
            (
                pltpu.make_async_remote_copy(
                    src_ref=source.at[slot],
                    dst_ref=target.at[slot],
                    send_sem=sent.at[slot],
                    recv_sem=received.at[slot],
                    device_id=(me + side * offset,),
                    device_id_type=MESH,
                ),
                on_axis(side * offset),
                on_axis(-side * offset),
            )
            for slot, offset in enumerate(OFFSETS)
        ]

    def start(copies):
        for copy, to, _ in copies:
            pl.when(to)(copy.start)

    def wait_recv(copies):
        for copy, _, come in copies:
            pl.when(come)(copy.wait_recv)

    def wait_send(copies):
        for copy, to, _ in copies:
            pl.when(to)(copy.wait_send)

    side = DOFS * ROWS
    tall = lax.broadcasted_iota(jnp.int32, (side, DOFS), 0) // ROWS
    unknown = lax.broadcasted_iota(jnp.int32, (side, DOFS), 1)
    repeat = jnp.where(tall == unknown, 1.0, 0.0).astype(jnp.bfloat16)
    row_step = lax.broadcasted_iota(jnp.int32, (side, 2 * side), 0) & (ROWS - 1)
    twice = jnp.concatenate([repeat, repeat], axis=0)
    column_step = lax.broadcasted_iota(jnp.int32, (side, 2 * side), 1) & (ROWS - 1)
    whole = stiff[...]
    top = whole.astype(jnp.bfloat16)
    for number, part in enumerate((top, (whole - top.astype(jnp.float32)).astype(jnp.bfloat16))):
        rows = jnp.dot(repeat, part, preferred_element_type=jnp.float32).astype(jnp.bfloat16)
        full = lax.dot_general(
            rows, twice, (((1,), (1,)), ((), ())), preferred_element_type=jnp.float32
        )
        kron[number] = jnp.where(row_step == column_step, full, 0.0).astype(jnp.bfloat16)

    for row in range(inner_rows):
        cut = slice(row * LANES, (row + 1) * LANES)
        face_a[row : row + 1, :] = inner[0:1, cut]
        face_b[row : row + 1, :] = inner[1:2, cut]
    for row in range(cross_rows):
        cut = slice(row * LANES, (row + 1) * LANES)
        face_a[inner_rows + row : inner_rows + row + 1, :] = cross[0:1, cut]
        face_b[inner_rows + row : inner_rows + row + 1, :] = cross[1:2, cut]

    out_perm[...] = jnp.zeros(out_perm.shape, jnp.float32)

    def inner_faces(step):
        base = pl.multiple_of(step * ROWS, ROWS)
        where_a = face_a[pl.ds(base, ROWS), :]
        where_b = face_b[pl.ds(base, ROWS), :]
        products = []
        others = [where_b[row : row + 1] for row in range(ROWS)]
        others = multiply(cell_parts, others, 2, cell_blocks // 2)
        for row in range(ROWS):
            pa, qa = gather(cell_planes, spread(where_a[row : row + 1]), 0, cell_blocks)
            pb, qb = others[row]
            products.append(jnp.sum((pa - pb) * (qa - qb), axis=0, keepdims=True))
        product = jnp.concatenate(products, axis=0)
        perm_a = gather(perm_plane, where_a, 0, cell_blocks)[0]
        perm_b = gather(perm_plane, where_b, 0, cell_blocks)[0]
        return face_terms(product, perm_a, perm_b), (where_a, where_b)

    def keep(lanes, values, corner):
        for comp in range(3):
            base = (comp * 8 + corner) * ROWS
            near = slice(base, base + 2 * ROWS)
            both = jnp.concatenate([value[comp] for value in values], axis=0)
            top = both.astype(jnp.bfloat16)
            low = (both - top.astype(jnp.float32)).astype(jnp.bfloat16)
            forward[near, lanes] = top
            forward[DOFS * ROWS + base : DOFS * ROWS + base + 2 * ROWS, lanes] = low
            adjoint[near, lanes] = jnp.concatenate([value[3 + comp] for value in values], axis=0)

    def inner_elements(step):
        lanes = pl.ds(pl.multiple_of(step * LANES, LANES), LANES)
        for corner in range(0, 8, 2):
            rows = [elem[one : one + 1, lanes] for one in (corner, corner + 1)]
            if corner < 6:
                values = multiply(parts, rows, 6, node_blocks // 2)
            else:
                values = [gather(planes, spread(row), 0, node_blocks) for row in rows]
            keep(lanes, values, corner)

    face_steps = inner_rows // ROWS // 2
    inner_blocks = elem_blocks - edge_blocks
    each = inner_blocks // face_steps
    assert 2 * face_steps * ROWS == inner_rows and each * face_steps == inner_blocks

    def inner(step, carry):
        for half in range(2):
            terms, where = inner_faces(2 * step + half)
            for number in range(each // 2):
                inner_elements(step * each + half * (each // 2) + number)
                if number == 0:
                    out_perm[...] += scatter(terms, where, cell_blocks)
        return carry

    early = jnp.logical_not(on_axis(-2))
    first = jnp.where(early, 1, 0)
    second = jnp.where(early, 3, 2)
    lax.fori_loop(0, first, inner, 0)

    pl.semaphore_wait(barrier, around)
    cell_copies = exchange(cell_box, ghost_cells, cell_send, cell_recv, -1)
    node_copies = exchange(node_box, ghost_nodes, node_send, node_recv, -1)
    start(cell_copies)
    start(node_copies)

    lax.fori_loop(first, second, inner, 0)

    wide = elem.shape[1] // 4

    def strains(part):
        lanes = slice(part * wide, (part + 1) * wide)
        weighted = jnp.dot(kron[0], forward[:, lanes], preferred_element_type=jnp.float32)
        weighted += jnp.dot(
            kron[1, :, :side], forward[:side, lanes], preferred_element_type=jnp.float32
        )
        product = weighted * adjoint[:, lanes]
        sums = jnp.sum(product, axis=0, keepdims=True)
        for row in range(wide // LANES):
            spot = part * (wide // LANES) + row
            strain[spot : spot + 1, :] = sums[:, row * LANES : (row + 1) * LANES]

    wait_recv(cell_copies)

    def ghosts(source, number):
        return lambda block: source[block, number]

    where_a = face_a[inner_rows : inner_rows + cross_rows, :]
    where_b = face_b[inner_rows : inner_rows + cross_rows, :]
    products = []
    own = [where_a[row : row + 1] for row in range(cross_rows)]
    own = multiply(cell_parts, own, 2, cell_blocks // 2)
    for row in range(cross_rows):
        pa, qa = own[row]
        pb, qb = gather([ghosts(ghost_cells, 0), ghosts(ghost_cells, 1)], spread(where_b[row : row + 1]), 0, slots)
        products.append(jnp.sum((pa - pb) * (qa - qb), axis=0, keepdims=True))
    product = jnp.concatenate(products, axis=0)
    perm_a = gather(perm_plane, where_a, 0, cell_blocks)[0]
    perm_b = gather([ghosts(ghost_cells, 2)], where_b, 0, slots)[0]
    term_a, term_b = face_terms(product, perm_a, perm_b)
    strains(0)
    owed = scatter([term_b], [where_b], slots)
    for slot in range(slots):
        back[slot] = owed[slot : slot + 1, :]
    strains(1)
    out_perm[...] += scatter([term_a], [where_a], cell_blocks)
    backs = exchange(back, returned, back_send, back_recv, 1)
    start(backs)

    lax.fori_loop(second, face_steps, inner, 0)

    wait_recv(node_copies)
    far_planes = [ghosts(ghost_nodes, number) for number in range(6)]

    def edge_elements(step):
        lanes = pl.ds(pl.multiple_of(step * LANES, LANES), LANES)
        for corner in range(0, 8, 2):
            values = []
            rows = [elem[one : one + 1, lanes] for one in (corner, corner + 1)]
            near = multiply(parts, rows, 6, node_blocks // 2)
            for row, mine in zip(rows, near):
                index = spread(row)
                far = gather(far_planes, index - node_blocks * LANES, 0, slots)
                inside = index < node_blocks * LANES
                values.append([jnp.where(inside, a, b) for a, b in zip(mine, far)])
            keep(lanes, values, corner)

    for number in range(edge_blocks):
        edge_elements(inner_blocks + number)
    wait_recv(backs)
    arrived = jnp.concatenate([returned[slot] for slot in range(slots)], axis=0)
    strains(2)
    strains(3)
    out_perm[...] += scatter([arrived], [send_cells[...]], cell_blocks)
    out_young[...] = -youngs[...] * strain[...]
    wait_send(cell_copies)
    wait_send(node_copies)
    wait_send(backs)


def deliver(both, young, flow, sem):
    copies = [
        pltpu.make_async_copy(both.at[number], target, sem.at[number])
        for number, target in enumerate((young, flow))
    ]
    for copy in copies:
        copy.start()
    for copy in copies:
        copy.wait()


def on_device(count, *arguments):
    (disp, adj, press, adjpress, youngs, perm, stiff, nodes, cells, elem, inner, cross) = arguments
    blocks = youngs.shape[0] // LANES
    slots = len(OFFSETS)
    face_rows = (inner.shape[1] + cross.shape[1]) // LANES
    vmem = pl.BlockSpec(memory_space=pltpu.VMEM)
    tile = (ROWS, LANES)
    shape = jax.ShapeDtypeStruct((blocks, LANES), jnp.float32)
    operands = (
        disp.transpose(1, 0, 2),
        adj.transpose(1, 0, 2),
        press,
        adjpress,
        youngs.reshape(blocks, LANES),
        perm.reshape(blocks, LANES),
        stiff,
        nodes,
        cells,
        elem,
        inner,
        cross,
    )
    both = pl.pallas_call(
        functools.partial(kernel, count),
        out_shape=pltpu.VMEM((2, blocks, LANES), jnp.float32),
        in_specs=[pl.BlockSpec(memory_space=pltpu.HBM)] * 12,
        out_specs=vmem,
        scratch_shapes=[pltpu.VMEM(one.shape, one.dtype) for one in operands]
        + [
            pltpu.VMEM((disp.shape[2] // WIDE * 6 * ROWS, 2 * WIDE), jnp.bfloat16),
            pltpu.VMEM((blocks // 2 * 2 * ROWS, 2 * WIDE), jnp.bfloat16),
            pltpu.VMEM((blocks,) + tile, jnp.float32),
            pltpu.VMEM((slots, 6) + tile, jnp.float32),
            pltpu.VMEM((slots, 3) + tile, jnp.float32),
            pltpu.VMEM((slots, 6) + tile, jnp.float32),
            pltpu.VMEM((slots, 3) + tile, jnp.float32),
            pltpu.VMEM((slots, 1, LANES), jnp.float32),
            pltpu.VMEM((slots, 1, LANES), jnp.float32),
            pltpu.VMEM((2 * DOFS * ROWS, elem.shape[1]), jnp.bfloat16),
            pltpu.VMEM((DOFS * ROWS, elem.shape[1]), jnp.float32),
            pltpu.VMEM((2, DOFS * ROWS, 2 * DOFS * ROWS), jnp.bfloat16),
            pltpu.VMEM((elem.shape[1] // LANES, LANES), jnp.float32),
            pltpu.VMEM((face_rows, LANES), jnp.int32),
            pltpu.VMEM((face_rows, LANES), jnp.int32),
            pltpu.SemaphoreType.DMA((slots,)),
            pltpu.SemaphoreType.DMA((slots,)),
            pltpu.SemaphoreType.DMA((slots,)),
            pltpu.SemaphoreType.DMA((slots,)),
            pltpu.SemaphoreType.DMA((slots,)),
            pltpu.SemaphoreType.DMA((slots,)),
            pltpu.SemaphoreType.DMA((len(operands),)),
        ],
        compiler_params=pltpu.CompilerParams(
            collective_id=0, has_side_effects=True),
    )(*operands)
    size = blocks * LANES
    whole = jax.ShapeDtypeStruct((blocks, LANES), jnp.float32)
    anywhere = pl.BlockSpec(memory_space=pl.ANY)
    young, flow = pl.pallas_call(
        deliver,
        out_shape=(whole, whole),
        in_specs=[vmem],
        out_specs=(anywhere, anywhere),
        scratch_shapes=[pltpu.SemaphoreType.DMA((2,))],
        compiler_params=pltpu.CompilerParams(vmem_limit_bytes=2**20),
    )(both)
    return (young.reshape(-1), flow.reshape(-1))


def solution(mesh):
    in_specs = (
        P(None, None, "dom"),
        P(None, None, "dom"),
        P(None, "dom"),
        P(None, "dom"),
        P("dom"),
        P("dom"),
        P(),
        P(None, "dom"),
        P(None, "dom"),
        P(None, "dom"),
        P(None, "dom"),
        P(None, "dom"),
    )
    out_specs = (P("dom"), P("dom"))
    return jax.shard_map(
        functools.partial(on_device, mesh.shape["dom"]),
        mesh=mesh,
        in_specs=in_specs,
        out_specs=out_specs,
        check_vma=False,
    )
```

```python
import functools

import jax
import jax.numpy as jnp
from jax import lax
from jax.experimental import pallas as pl
from jax.experimental.pallas import tpu as pltpu
from jax.sharding import PartitionSpec as P

OFFSETS = (1, -1, 2, -2, 4, -4, 8, -8)
MESH = pl.DeviceIdType.MESH
LANES = 128
ROWS = 8
DOFS = 24
WIDE = 256
EIGHT = jnp.float8_e4m3fn
SCALE = 256.0
STEPS = (1.0, 16.0, 512.0)


def pick(table, lo):
    return jnp.take_along_axis(table, lo, axis=1, mode="promise_in_bounds")


def spread(row):
    return jnp.broadcast_to(row, (ROWS, LANES))


def gather(tables, index, first, last):
    lo = index & (LANES - 1)
    hi = index >> 7
    out = None
    for block in range(first, last):
        got = [pick(table(block), lo) for table in tables]
        if out is None:
            out = got
        else:
            here = hi == block
            out = [jnp.where(here, new, old) for new, old in zip(got, out)]
    return out


def onehot(index):
    rows = lax.broadcasted_iota(jnp.int32, (WIDE, LANES), 0).astype(jnp.bfloat16)
    low = (index & (WIDE - 1)).astype(jnp.float32).astype(jnp.bfloat16)
    same = rows == jnp.broadcast_to(low, (WIDE, LANES))
    hot = jnp.where(same, jnp.bfloat16(1), jnp.bfloat16(0))
    return jnp.concatenate([hot, hot], axis=0)


def weighted(index):
    rows = lax.broadcasted_iota(jnp.int32, (WIDE, LANES), 0).astype(jnp.bfloat16)
    low = (index & (WIDE - 1)).astype(jnp.float32).astype(jnp.bfloat16)
    same = rows == jnp.broadcast_to(low, (WIDE, LANES))
    hots = [jnp.where(same, jnp.bfloat16(SCALE / step), jnp.bfloat16(0)) for step in STEPS]
    return jnp.concatenate([hot.astype(EIGHT) for hot in hots], axis=0)


def fill_nodes(parts, planes, blocks):
    height = 2 * len(planes) * ROWS
    for block in range(0, blocks, 2):
        rest = SCALE * jnp.concatenate(
            [
                jnp.concatenate([plane(2 * near), plane(2 * near + 1)], axis=1)
                for near in (block, block + 1)
                for plane in planes
            ],
            axis=0,
        )
        base = block // 2 * height
        for number, step in enumerate(STEPS):
            top = (step * rest).astype(EIGHT)
            parts[base : base + height, number * WIDE : (number + 1) * WIDE] = top
            rest = rest - top.astype(jnp.float32) * (1 / step)


def fill(parts, planes, blocks):
    for block in range(blocks):
        for number in range(0, len(planes), 2):
            both = jnp.concatenate(
                [
                    jnp.concatenate([plane(2 * block), plane(2 * block + 1)], axis=1)
                    for plane in planes[number : number + 2]
                ],
                axis=0,
            )
            top = both.astype(jnp.bfloat16)
            base = (block * len(planes) + number) * ROWS
            parts[base : base + 2 * ROWS, :WIDE] = top
            parts[base : base + 2 * ROWS, WIDE:] = (both - top.astype(jnp.float32)).astype(
                jnp.bfloat16
            )


def multiply(parts, indices, planes, blocks, hot=onehot, scale=None):
    right = jnp.concatenate([hot(index) for index in indices], axis=1)
    got = jnp.dot(parts[...], right, preferred_element_type=jnp.float32)
    answers = []
    for number, index in enumerate(indices):
        hi = spread(index) >> 8
        mine = got[:, number * LANES : (number + 1) * LANES]
        out = [mine[plane * ROWS : (plane + 1) * ROWS] for plane in range(planes)]
        for block in range(1, blocks):
            here = hi == block
            for plane in range(planes):
                base = (block * planes + plane) * ROWS
                out[plane] = jnp.where(here, mine[base : base + ROWS], out[plane])
        if scale is not None:
            out = [scale * one for one in out]
        answers.append(out)
    return answers


def scatter(terms, index, height):
    sub_hi = lax.broadcasted_iota(jnp.int32, (height, LANES), 0)
    sub_lo = lax.broadcasted_iota(jnp.int32, (LANES, LANES), 0).astype(jnp.bfloat16)
    left, right = [], []
    for term, where in zip(terms, index):
        top = term.astype(jnp.bfloat16).astype(jnp.float32)
        rest = term - top
        middle = rest.astype(jnp.bfloat16).astype(jnp.float32)
        low = rest - middle
        hi = where >> 7
        lo = (where & (LANES - 1)).astype(jnp.float32)
        for row in range(ROWS):
            cut = slice(row, row + 1)
            mask = jnp.broadcast_to(hi[cut], (height, LANES)) == sub_hi
            parts = [
                jnp.where(mask, jnp.broadcast_to(part[cut], (height, LANES)), 0.0)
                for part in (top, middle, low)
            ]
            left.append(jnp.concatenate(parts, axis=0).astype(jnp.bfloat16))
            same = jnp.broadcast_to(lo[cut].astype(jnp.bfloat16), (LANES, LANES)) == sub_lo
            right.append(jnp.where(same, jnp.bfloat16(1), jnp.bfloat16(0)))
    sums = lax.dot_general(
        jnp.concatenate(left, axis=1),
        jnp.concatenate(right, axis=1),
        (((1,), (1,)), ((), ())),
        preferred_element_type=jnp.float32,
    )
    return sums[:height] + sums[height : 2 * height] + sums[2 * height :]


def face_terms(product, perm_a, perm_b):
    total = perm_a + perm_b
    common = 2.0 * perm_a * perm_b * product / (total * total)
    return common * perm_b, common * perm_a


def kernel(count, *refs):
    arguments, refs = refs[:12], refs[12:]
    out, refs = refs[0], refs[1:]
    out_young, out_perm = out.at[0], out.at[1]
    (disp, adj, press, adjpress, youngs, perm), refs = refs[:6], refs[6:]
    (stiff, send_nodes, send_cells, elem, inner, cross), refs = refs[:6], refs[6:]
    (
    parts,
    cell_parts,
    permtab,
    node_box,
    cell_box,
    ghost_nodes,
    ghost_cells,
    back,
    returned,
    forward,
    adjoint,
    kron,
    strain,
    face_a,
    face_b,
    node_send,
    node_recv,
    cell_send,
    cell_recv,
 back_send,
    back_recv,
    load_sem,
    ) = refs
    held = (disp, adj, press, adjpress, youngs, perm)
    held += (stiff, send_nodes, send_cells, elem, inner, cross)
    loads = [
        pltpu.make_async_copy(source, target, load_sem.at[number])
        for number, (source, target) in enumerate(zip(arguments, held))
    ]
    for load in loads:
        load.start()
    me = lax.axis_index("dom")
    slots = len(OFFSETS)
    node_blocks = disp.shape[2] // LANES
    cell_blocks = perm.shape[0]
    elem_blocks = elem.shape[1] // LANES
    edge_blocks = elem_blocks // 4
    inner_rows = inner.shape[1] // LANES
    cross_rows = cross.shape[1] // LANES

    def on_axis(steps):
        return (me + steps >= 0) & (me + steps < count)

    barrier = pltpu.get_barrier_semaphore()
    around = 0
    for slot, offset in enumerate(OFFSETS):
        around += on_axis(offset).astype(jnp.int32)

        @pl.when(on_axis(offset))
        def _():
            pl.semaphore_signal(barrier, inc=1, device_id=(me + offset,), device_id_type=MESH)

        @pl.when(jnp.logical_not(on_axis(-offset)))
        def _():
            returned[slot] = jnp.zeros((1, LANES), jnp.float32)

    def plane(number):
        source, comp = (disp, number) if number < 3 else (adj, number - 3)
        return lambda block: source[comp, :, block * LANES : (block + 1) * LANES]

    def cells(source):
        return lambda block: source[:, block * LANES : (block + 1) * LANES]

    planes = [plane(number) for number in range(6)]
    cell_planes = [cells(press), cells(adjpress)]
    perm_plane = [lambda block: permtab[block]]

    for number in (2, 3, 7, 8, 5, 0, 1, 6, 9, 10, 11, 4):
        loads[number].wait()

    for block in range(cell_blocks):
        permtab[block] = spread(perm[block : block + 1, :])
    fill_nodes(parts, planes, node_blocks // 2)

    def nodes_at(rows):
        return multiply(parts, rows, 6, node_blocks // 2, weighted, SCALE**-2)

    fill(cell_parts, cell_planes, cell_blocks // 2)
    for pair in range(0, slots, 2):
        rows = [send_nodes[slot : slot + 1, :] for slot in (pair, pair + 1)]
        nodes = nodes_at(rows)
        for slot in (pair, pair + 1):
            where = spread(send_cells[slot : slot + 1, :])
            values = gather(cell_planes, where, 0, cell_blocks)
            for number, value in enumerate(nodes[slot - pair]):
                node_box[slot, number] = value
            for number, value in enumerate(values):
                cell_box[slot, number] = value
    sent_perm = gather(perm_plane, send_cells[...], 0, cell_blocks)[0]
    for slot in range(slots):
        cell_box[slot, 2] = spread(sent_perm[slot : slot + 1, :])

    def exchange(source, target, sent, received, side):
        return [
            (
                pltpu.make_async_remote_copy(
                    src_ref=source.at[slot],
                    dst_ref=target.at[slot],
                    send_sem=sent.at[slot],
                    recv_sem=received.at[slot],
                    device_id=(me + side * offset,),
                    device_id_type=MESH,
                ),
                on_axis(side * offset),
                on_axis(-side * offset),
            )
            for slot, offset in enumerate(OFFSETS)
        ]

    def start(copies):
        for copy, to, _ in copies:
            pl.when(to)(copy.start)

    def wait_recv(copies):
        for copy, _, come in copies:
            pl.when(come)(copy.wait_recv)

    def wait_send(copies):
        for copy, to, _ in copies:
            pl.when(to)(copy.wait_send)

    side = DOFS * ROWS
    tall = lax.broadcasted_iota(jnp.int32, (side, DOFS), 0) // ROWS
    unknown = lax.broadcasted_iota(jnp.int32, (side, DOFS), 1)
    repeat = jnp.where(tall == unknown, 1.0, 0.0).astype(jnp.bfloat16)
    row_step = lax.broadcasted_iota(jnp.int32, (side, 2 * side), 0) & (ROWS - 1)
    twice = jnp.concatenate([repeat, repeat], axis=0)
    column_step = lax.broadcasted_iota(jnp.int32, (side, 2 * side), 1) & (ROWS - 1)
    whole = stiff[...]
    top = whole.astype(jnp.bfloat16)
    for number, part in enumerate((top, (whole - top.astype(jnp.float32)).astype(jnp.bfloat16))):
        rows = jnp.dot(repeat, part, preferred_element_type=jnp.float32).astype(jnp.bfloat16)
        full = lax.dot_general(
            rows, twice, (((1,), (1,)), ((), ())), preferred_element_type=jnp.float32
        )
        kron[number] = jnp.where(row_step == column_step, full, 0.0).astype(jnp.bfloat16)

    for row in range(inner_rows):
        cut = slice(row * LANES, (row + 1) * LANES)
        face_a[row : row + 1, :] = inner[0:1, cut]
        face_b[row : row + 1, :] = inner[1:2, cut]
    for row in range(cross_rows):
        cut = slice(row * LANES, (row + 1) * LANES)
        face_a[inner_rows + row : inner_rows + row + 1, :] = cross[0:1, cut]
        face_b[inner_rows + row : inner_rows + row + 1, :] = cross[1:2, cut]

    out_perm[...] = jnp.zeros(out_perm.shape, jnp.float32)

    def inner_faces(step):
        base = pl.multiple_of(step * ROWS, ROWS)
        where_a = face_a[pl.ds(base, ROWS), :]
        where_b = face_b[pl.ds(base, ROWS), :]
        products = []
        others = [where_b[row : row + 1] for row in range(ROWS)]
        others = multiply(cell_parts, others, 2, cell_blocks // 2)
        for row in range(ROWS):
            pa, qa = gather(cell_planes, spread(where_a[row : row + 1]), 0, cell_blocks)
            pb, qb = others[row]
            products.append(jnp.sum((pa - pb) * (qa - qb), axis=0, keepdims=True))
        product = jnp.concatenate(products, axis=0)
        perm_a = gather(perm_plane, where_a, 0, cell_blocks)[0]
        perm_b = gather(perm_plane, where_b, 0, cell_blocks)[0]
        return face_terms(product, perm_a, perm_b), (where_a, where_b)

    def keep(lanes, values, corner):
        for comp in range(3):
            base = (comp * 8 + corner) * ROWS
            near = slice(base, base + 2 * ROWS)
            both = jnp.concatenate([value[comp] for value in values], axis=0)
            top = both.astype(jnp.bfloat16)
            low = (both - top.astype(jnp.float32)).astype(jnp.bfloat16)
            forward[near, lanes] = top
            forward[DOFS * ROWS + base : DOFS * ROWS + base + 2 * ROWS, lanes] = low
            adjoint[near, lanes] = jnp.concatenate([value[3 + comp] for value in values], axis=0)

    def inner_elements(step):
        lanes = pl.ds(pl.multiple_of(step * LANES, LANES), LANES)
        for corner in range(0, 8, 2):
            rows = [elem[one : one + 1, lanes] for one in (corner, corner + 1)]
            if corner < 6:
                values = nodes_at(rows)
            else:
                values = [gather(planes, spread(row), 0, node_blocks) for row in rows]
            keep(lanes, values, corner)

    face_steps = inner_rows // ROWS // 2
    inner_blocks = elem_blocks - edge_blocks
    each = inner_blocks // face_steps
    assert 2 * face_steps * ROWS == inner_rows and each * face_steps == inner_blocks

    def inner(step, carry):
        for half in range(2):
            terms, where = inner_faces(2 * step + half)
            for number in range(each // 2):
                inner_elements(step * each + half * (each // 2) + number)
                if number == 0:
                    out_perm[...] += scatter(terms, where, cell_blocks)
        return carry

    early = jnp.logical_not(on_axis(-2))
    first = jnp.where(early, 1, 0)
    second = jnp.where(early, 3, 2)
    lax.fori_loop(0, first, inner, 0)

    pl.semaphore_wait(barrier, around)
    cell_copies = exchange(cell_box, ghost_cells, cell_send, cell_recv, -1)
    node_copies = exchange(node_box, ghost_nodes, node_send, node_recv, -1)
    start(cell_copies)
    start(node_copies)

    lax.fori_loop(first, second, inner, 0)

    wide = elem.shape[1] // 4

    def strains(part):
        lanes = slice(part * wide, (part + 1) * wide)
        weighted = jnp.dot(kron[0], forward[:, lanes], preferred_element_type=jnp.float32)
        weighted += jnp.dot(
            kron[1, :, :side], forward[:side, lanes], preferred_element_type=jnp.float32
        )
        product = weighted * adjoint[:, lanes]
        sums = jnp.sum(product, axis=0, keepdims=True)
        for row in range(wide // LANES):
            spot = part * (wide // LANES) + row
            strain[spot : spot + 1, :] = sums[:, row * LANES : (row + 1) * LANES]

    wait_recv(cell_copies)

    def ghosts(source, number):
        return lambda block: source[block, number]

    where_a = face_a[inner_rows : inner_rows + cross_rows, :]
    where_b = face_b[inner_rows : inner_rows + cross_rows, :]
    products = []
    own = [where_a[row : row + 1] for row in range(cross_rows)]
    own = multiply(cell_parts, own, 2, cell_blocks // 2)
    for row in range(cross_rows):
        pa, qa = own[row]
        pb, qb = gather([ghosts(ghost_cells, 0), ghosts(ghost_cells, 1)], spread(where_b[row : row + 1]), 0, slots)
        products.append(jnp.sum((pa - pb) * (qa - qb), axis=0, keepdims=True))
    product = jnp.concatenate(products, axis=0)
    perm_a = gather(perm_plane, where_a, 0, cell_blocks)[0]
    perm_b = gather([ghosts(ghost_cells, 2)], where_b, 0, slots)[0]
    term_a, term_b = face_terms(product, perm_a, perm_b)
    strains(0)
    owed = scatter([term_b], [where_b], slots)
    for slot in range(slots):
        back[slot] = owed[slot : slot + 1, :]
    strains(1)
    out_perm[...] += scatter([term_a], [where_a], cell_blocks)
    backs = exchange(back, returned, back_send, back_recv, 1)
    start(backs)

    lax.fori_loop(second, face_steps, inner, 0)

    wait_recv(node_copies)
    far_planes = [ghosts(ghost_nodes, number) for number in range(6)]

    def edge_elements(step):
        lanes = pl.ds(pl.multiple_of(step * LANES, LANES), LANES)
        for corner in range(0, 8, 2):
            values = []
            rows = [elem[one : one + 1, lanes] for one in (corner, corner + 1)]
            near = nodes_at(rows)
            for row, mine in zip(rows, near):
                index = spread(row)
                far = gather(far_planes, index - node_blocks * LANES, 0, slots)
                inside = index < node_blocks * LANES
                values.append([jnp.where(inside, a, b) for a, b in zip(mine, far)])
            keep(lanes, values, corner)

    for number in range(edge_blocks):
        edge_elements(inner_blocks + number)
    strains(2)
    strains(3)
    out_young[...] = -youngs[...] * strain[...]
    wait_recv(backs)
    arrived = jnp.concatenate([returned[slot] for slot in range(slots)], axis=0)
    out_perm[...] += scatter([arrived], [send_cells[...]], cell_blocks)
    wait_send(cell_copies)
    wait_send(node_copies)
    wait_send(backs)


def deliver(both, young, flow, sem):
    copies = [
        pltpu.make_async_copy(both.at[number], target, sem.at[number])
        for number, target in enumerate((young, flow))
    ]
    for copy in copies:
        copy.start()
    for copy in copies:
        copy.wait()


def on_device(count, *arguments):
    (disp, adj, press, adjpress, youngs, perm, stiff, nodes, cells, elem, inner, cross) = arguments
    blocks = youngs.shape[0] // LANES
    slots = len(OFFSETS)
    face_rows = (inner.shape[1] + cross.shape[1]) // LANES
    vmem = pl.BlockSpec(memory_space=pltpu.VMEM)
    tile = (ROWS, LANES)
    shape = jax.ShapeDtypeStruct((blocks, LANES), jnp.float32)
    operands = (
        disp.transpose(1, 0, 2),
        adj.transpose(1, 0, 2),
        press,
        adjpress,
        youngs.reshape(blocks, LANES),
        perm.reshape(blocks, LANES),
        stiff,
        nodes,
        cells,
        elem,
        inner,
        cross,
    )
    both = pl.pallas_call(
        functools.partial(kernel, count),
        out_shape=pltpu.VMEM((2, blocks, LANES), jnp.float32),
        in_specs=[pl.BlockSpec(memory_space=pltpu.HBM)] * 12,
        out_specs=vmem,
        scratch_shapes=[pltpu.VMEM(one.shape, one.dtype) for one in operands]
        + [
            pltpu.VMEM((disp.shape[2] // WIDE * 6 * ROWS, len(STEPS) * WIDE), EIGHT),
            pltpu.VMEM((blocks // 2 * 2 * ROWS, 2 * WIDE), jnp.bfloat16),
            pltpu.VMEM((blocks,) + tile, jnp.float32),
            pltpu.VMEM((slots, 6) + tile, jnp.float32),
            pltpu.VMEM((slots, 3) + tile, jnp.float32),
            pltpu.VMEM((slots, 6) + tile, jnp.float32),
            pltpu.VMEM((slots, 3) + tile, jnp.float32),
            pltpu.VMEM((slots, 1, LANES), jnp.float32),
            pltpu.VMEM((slots, 1, LANES), jnp.float32),
            pltpu.VMEM((2 * DOFS * ROWS, elem.shape[1]), jnp.bfloat16),
            pltpu.VMEM((DOFS * ROWS, elem.shape[1]), jnp.float32),
            pltpu.VMEM((2, DOFS * ROWS, 2 * DOFS * ROWS), jnp.bfloat16),
            pltpu.VMEM((elem.shape[1] // LANES, LANES), jnp.float32),
            pltpu.VMEM((face_rows, LANES), jnp.int32),
            pltpu.VMEM((face_rows, LANES), jnp.int32),
            pltpu.SemaphoreType.DMA((slots,)),
            pltpu.SemaphoreType.DMA((slots,)),
            pltpu.SemaphoreType.DMA((slots,)),
            pltpu.SemaphoreType.DMA((slots,)),
            pltpu.SemaphoreType.DMA((slots,)),
            pltpu.SemaphoreType.DMA((slots,)),
            pltpu.SemaphoreType.DMA((len(operands),)),
        ],
        compiler_params=pltpu.CompilerParams(
            collective_id=0, has_side_effects=True),
    )(*operands)
    size = blocks * LANES
    whole = jax.ShapeDtypeStruct((blocks, LANES), jnp.float32)
    anywhere = pl.BlockSpec(memory_space=pl.ANY)
    young, flow = pl.pallas_call(
        deliver,
        out_shape=(whole, whole),
        in_specs=[vmem],
        out_specs=(anywhere, anywhere),
        scratch_shapes=[pltpu.SemaphoreType.DMA((2,))],
        compiler_params=pltpu.CompilerParams(vmem_limit_bytes=2**20),
    )(both)
    return (young.reshape(-1), flow.reshape(-1))


def solution(mesh):
    in_specs = (
        P(None, None, "dom"),
        P(None, None, "dom"),
        P(None, "dom"),
        P(None, "dom"),
        P("dom"),
        P("dom"),
        P(),
        P(None, "dom"),
        P(None, "dom"),
        P(None, "dom"),
        P(None, "dom"),
        P(None, "dom"),
    )
    out_specs = (P("dom"), P("dom"))
    return jax.shard_map(
        functools.partial(on_device, mesh.shape["dom"]),
        mesh=mesh,
        in_specs=in_specs,
        out_specs=out_specs,
        check_vma=False,
    )
```
